256 devices in a mesh: ctx: 32 (over x, z), pb: 2 (over core), ga: 4 (over y).
Axes of the slice: x: 4, y: 4, z: 8, core: 2. Of those that a mesh axis runs over, the one named last changes fastest.
Arguments:
- queries: bfloat16 [8192, 12288], P(('ctx', 'pb'), 'ga'), may hold values from -128 to 128
- stretch_keys: bfloat16 [8192, 768], P(('ctx', 'pb'), 'ga'), may hold values from -16 to 16
- stretch_values: bfloat16 [8192, 512], P(('ctx', 'pb'), 'ga'), may hold values from -6 to 6
- prior_cache_keys: bfloat16 [131072, 768], P('ctx', 'ga'), may hold values from -16 to 16
- cache_values: bfloat16 [131072, 512], P('ctx', 'ga'), may hold values from -6 to 6
- block_lengths: int32 [32, 256], P('ctx'), may hold values from 1 to 32, 4096 in all within a row
- compress_weights: float32 [4, 32], P('ga'), may hold values from 0.1 to 1.9
- selections: int32 [128, 4, 13], P(('ctx', 'pb'), 'ga'), may hold values from 1 to 2045, as said below
- gate_logits: float32 [3, 8192, 64], P(None, ('ctx', 'pb'), 'ga'), may hold values from -6 to 6
Outputs:
- attended: bfloat16 [8192, 8192], P(('ctx', 'pb'), 'ga')
The draws below stay inside these ranges and needn't reach their ends.
Inputs may be any that keep to these rules, and one draw needn't show every extreme that they name: `block_lengths`: each row belongs to one cache shard and sums to 4096; its largest entry is 32. `selections`: each row lists 13 different blocks, never the first or one of the last two blocks of a cache shard (a shard holds 64 blocks). Over the 2 rows of one device and one group at most 2 listed blocks lie in one cache shard, and for each group one cache shard holds exactly 2 of every device's listed blocks.
All inputs are finite; a program needn't handle non-finite values.
Results may differ from the reference program's by a relative error of at most 0.011.
Values may be sent and summed in bfloat16 or wider, within the bound.
A program may use at most 128 MiB of HBM per device.

```python
import math
import jax
import jax.numpy as jnp
import numpy as np
from jax import lax

HQ = 64
GROUPS = 4
DK = 192
DV = 128
CTX_DEV = 4096
QB_DEV = 2
QBLK = 64
SBLK = 64
TOPSEL = 16
NFIXED = 3
WINDOW = 512
CMAX = 32
CACHE_SHARDS = 32
QSHARDS = 64
CONTEXT = 131072
STRETCH = 8192
QBLOCKS = 128
BLK_DEV = 64
NBLK = 2048
NCB_DEV = 256
NCOMP = 8192
CAP = 2


def draw_queries(key, part):
    entries = jnp.clip(2.5 * jax.random.normal(jax.random.fold_in(key, 1), (STRETCH, HQ * DK), jnp.float32), -15.0, 15.0)
    return entries.astype(jnp.bfloat16)


def draw_prior_cache_keys(key, part):
    entries = jnp.clip(jax.random.normal(jax.random.fold_in(key, 2), (CONTEXT, GROUPS * DK), jnp.float32), -6.0, 6.0)
    return entries.astype(jnp.bfloat16)


def draw_stretch_keys(key, part):
    entries = jnp.clip(jax.random.normal(jax.random.fold_in(key, 3), (STRETCH, GROUPS * DK), jnp.float32), -6.0, 6.0)
    return entries.astype(jnp.bfloat16)


def draw_selections(key, part):
    listed = TOPSEL - NFIXED
    hot_shard = jax.random.randint(jax.random.fold_in(key, 11), (GROUPS,), 0, CACHE_SHARDS)

    def one_device(device_key, hot_owner):
        first_key, second_key, third_key = jax.random.split(device_key, 3)
        candidates = CACHE_SHARDS * CAP
        owners = jnp.arange(candidates, dtype=jnp.int32) // CAP
        copies = jnp.arange(candidates, dtype=jnp.int32) % CAP
        rank_draw = jax.random.permutation(first_key, candidates).astype(jnp.int32)
        priority = jnp.where(owners == hot_owner, copies - CAP, rank_draw)
        picked = jnp.argsort(priority, stable=True)[:QB_DEV * listed]
        offset_table = jax.vmap(lambda shard_key: jax.random.permutation(shard_key, BLK_DEV - 3)[:CAP])(jax.random.split(second_key, CACHE_SHARDS))
        picked_owner = owners[picked]
        block_ids = picked_owner * BLK_DEV + 1 + offset_table[picked_owner, copies[picked]].astype(jnp.int32)
        block_ids = jax.random.permutation(third_key, block_ids)
        return block_ids.reshape(QB_DEV, listed).astype(jnp.int32)
    device_keys = jax.random.split(jax.random.fold_in(key, 12), QSHARDS * GROUPS)
    owners_hot = jnp.tile(hot_shard, QSHARDS)
    drawn = jax.vmap(one_device)(device_keys, owners_hot)
    drawn = drawn.reshape(QSHARDS, GROUPS, QB_DEV, listed)
    return jnp.transpose(drawn, (0, 2, 1, 3)).reshape(QBLOCKS, GROUPS, listed)


def steps_of(key, dims, cuts, least, largest):
    gain, own = 1.0, jax.random.fold_in(key, 6)
    for axis_at, blocks in cuts:
        steps = jnp.exp(jax.random.uniform(jax.random.fold_in(own, axis_at), (blocks,), jnp.float32, least / len(cuts), largest / len(cuts)))
        gain = gain * jnp.repeat(steps, dims[axis_at] // blocks).reshape([-1 if axis == axis_at else 1 for axis in range(len(dims))])
    return gain


def profile(count, total, reach, lean):
    portions = [(1 << 20) // math.isqrt(rank ** lean) + 1 for rank in range(2, count + 1)]
    rest, holding = total - reach - (count - 1), [1] * (count - 1)
    while rest > 0:
        movable = [i for i in range(count - 1) if holding[i] < reach]
        pool, budget = sum([portions[i] for i in movable]), rest
        for i in movable:
            extra = min(reach - holding[i], max(1, budget * portions[i] // pool), rest)
            holding[i] = holding[i] + extra
            rest = rest - extra
    return np.array([reach] + holding)


def uneven_parts(rng, amount, total, limit, slope):
    if amount == 2:
        one = jax.random.randint(rng, (), max(1, total - limit), min(limit, total - 1) + 1)
        return jnp.stack([one, total - one])
    tallies = jnp.asarray(profile(amount, total, limit, slope), jnp.int32)
    twos = (amount - 1) // 2
    donor, taker = tallies[1:1 + 2 * twos:2], tallies[2:2 + 2 * twos:2]
    margin = jnp.minimum(donor - 1, limit - taker)
    shifted = jax.random.randint(jax.random.fold_in(rng, 1), (twos,), 0, 1 << 20) % (margin + 1)
    tallies = tallies.at[1:1 + 2 * twos:2].set(donor - shifted).at[2:2 + 2 * twos:2].set(taker + shifted)
    return tallies[jax.random.permutation(jax.random.fold_in(rng, 2), amount)]


def scatter_about(key, dims, scale, most, shards=(), kind=jnp.bfloat16):
    level = steps_of(key, dims, shards, -0.22, 0.18) if shards else 1.0
    values = jax.random.normal(key, dims, jnp.float32) * scale * level
    return jnp.minimum(jnp.maximum(values, -most), most).astype(kind)


def setup_inputs(seed: int = 0) -> dict:
    seeds = jax.random.split(jax.random.key(seed), 10)
    return {
        "queries": draw_queries(jax.random.fold_in(seeds[9], 71), 0),
        "stretch_keys": draw_stretch_keys(jax.random.fold_in(seeds[9], 71), 0),
        "stretch_values": scatter_about(seeds[2], (STRETCH, GROUPS * DV), 1.0, 6.0, ((0, 64), (1, 4))),
        "prior_cache_keys": draw_prior_cache_keys(jax.random.fold_in(seeds[9], 71), 0),
        "cache_values": scatter_about(seeds[4], (CONTEXT, GROUPS * DV), 1.0, 6.0, ((0, 32), (1, 4))),
        "block_lengths": jax.vmap(lambda own: uneven_parts(own, NCB_DEV, CTX_DEV, CMAX, 1))(jax.random.split(seeds[5], CACHE_SHARDS)).reshape((CACHE_SHARDS, NCB_DEV)).astype(jnp.int32),
        "compress_weights": jnp.clip(1.0 + 0.18 * jax.random.normal(seeds[6], (GROUPS, CMAX), jnp.float32), 0.1, 1.9),
        "selections": draw_selections(jax.random.fold_in(seeds[9], 71), 0),
        "gate_logits": scatter_about(seeds[8], (3, STRETCH, HQ), 1.5, 6.0, ((1, 64), (2, 4)), jnp.float32),
    }


floor_score = -1e+30

def compress_rows(cache_rows, value_rows, lengths, branch_weights):
    span = cache_rows.shape[0]
    starts = (jnp.cumsum(lengths) - lengths).astype(jnp.int32)
    positions = jnp.arange(span, dtype=jnp.int32)
    group_member = (positions[None, :] >= starts[:, None]) & (positions[None, :] < (starts + lengths)[:, None])
    offsets = lax.optimization_barrier(jnp.sum(jnp.where(group_member, positions[None, :] - starts[:, None], 0), axis=0)).astype(jnp.int32)
    lookup = jnp.arange(branch_weights.shape[0], dtype=jnp.int32)
    token_weight = lax.optimization_barrier(jnp.sum(jnp.where(offsets[:, None] == lookup[None, :], branch_weights[None, :], 0.0), axis=1))
    spread = 1.0 / jnp.sqrt(lengths.astype(jnp.float32))
    matrix = jnp.where(group_member, token_weight[None, :] * spread[:, None], 0.0).astype(jnp.bfloat16)
    packed_keys = jnp.dot(matrix.astype(jnp.float32), cache_rows.astype(jnp.float32), preferred_element_type=jnp.float32).astype(jnp.bfloat16)
    packed_values = jnp.dot(matrix.astype(jnp.float32), value_rows.astype(jnp.float32), preferred_element_type=jnp.float32).astype(jnp.bfloat16)
    return (packed_keys, packed_values)

def softmax_mix(scores, value_rows):
    row_peak = lax.optimization_barrier(jnp.max(scores, axis=1, keepdims=True))
    branch_weights = jnp.exp(scores - row_peak)
    row_total = lax.optimization_barrier(jnp.sum(branch_weights, axis=1, keepdims=True))
    return jnp.dot(branch_weights.astype(jnp.bfloat16).astype(jnp.float32), value_rows.astype(jnp.float32), preferred_element_type=jnp.float32) / row_total

def reference(queries, stretch_keys, stretch_values, prior_cache_keys, cache_values, block_lengths, compress_weights, selections, gate_logits):
    head_count = HQ // GROUPS
    score_scale = 1.0 / math.sqrt(DK)
    always_on = jnp.array([0, NBLK - 2, NBLK - 1], dtype=jnp.int32)
    near_range = jnp.arange(WINDOW + QBLK, dtype=jnp.int32)
    query_range = jnp.arange(QBLK, dtype=jnp.int32)
    results = []
    for group_index in range(GROUPS):
        group_keys = prior_cache_keys[:, group_index * DK:(group_index + 1) * DK]
        group_values = cache_values[:, group_index * DV:(group_index + 1) * DV]
        weight_row = compress_weights[group_index]
        packed_keys, packed_values = lax.map(lambda operand: compress_rows(operand[0], operand[1], operand[2], weight_row), (group_keys.reshape(CACHE_SHARDS, CTX_DEV, DK), group_values.reshape(CACHE_SHARDS, CTX_DEV, DV), block_lengths))
        packed_keys = packed_keys.reshape(NCOMP, DK)
        packed_values = packed_values.reshape(NCOMP, DV)
        key_blocks = group_keys.reshape(NBLK, SBLK, DK)
        value_blocks = group_values.reshape(NBLK, SBLK, DV)
        padded_keys = jnp.concatenate([jnp.zeros((WINDOW, DK), jnp.bfloat16), stretch_keys[:, group_index * DK:(group_index + 1) * DK]], axis=0)
        padded_values = jnp.concatenate([jnp.zeros((WINDOW, DV), jnp.bfloat16), stretch_values[:, group_index * DV:(group_index + 1) * DV]], axis=0)
        group_queries = queries[:, group_index * head_count * DK:(group_index + 1) * head_count * DK].reshape(QBLOCKS, QBLK * head_count, DK)
        group_lists = selections[:, group_index, :]

        def one_block(operand):
            query_rows, listed, block_index = operand
            compressed = softmax_mix(jnp.dot(query_rows.astype(jnp.float32), packed_keys.T.astype(jnp.float32), preferred_element_type=jnp.float32) * score_scale, packed_values)
            chosen = jnp.concatenate([always_on, listed.astype(jnp.int32)])
            selected_keys = jnp.take(key_blocks, chosen, axis=0).reshape(TOPSEL * SBLK, DK)
            chosen_values = jnp.take(value_blocks, chosen, axis=0).reshape(TOPSEL * SBLK, DV)
            selected = softmax_mix(jnp.dot(query_rows.astype(jnp.float32), selected_keys.T.astype(jnp.float32), preferred_element_type=jnp.float32) * score_scale, chosen_values)
            starting_position = (block_index * QBLK).astype(jnp.int32)
            near_keys = lax.dynamic_slice_in_dim(padded_keys, starting_position, WINDOW + QBLK, 0)
            near_values = lax.dynamic_slice_in_dim(padded_values, starting_position, WINDOW + QBLK, 0)
            key_pos = starting_position - WINDOW + near_range
            query_pos = starting_position + query_range
            distance = query_pos[:, None] - key_pos[None, :]
            allowed = (distance >= 0) & (distance < WINDOW) & (key_pos[None, :] >= 0)
            allowed = jnp.repeat(allowed, head_count, axis=0)
            near_scores = jnp.dot(query_rows.astype(jnp.float32), near_keys.T.astype(jnp.float32), preferred_element_type=jnp.float32) * score_scale
            windowed = softmax_mix(jnp.where(allowed, near_scores, floor_score), near_values)
            return (compressed, selected, windowed)
        branches = lax.map(one_block, (group_queries, group_lists, jnp.arange(QBLOCKS, dtype=jnp.int32)))
        compressed_out = branches[0].reshape(STRETCH, head_count, DV)
        selected_out = branches[1].reshape(STRETCH, head_count, DV)
        windowed_out = branches[2].reshape(STRETCH, head_count, DV)
        gate_values = jax.nn.sigmoid(gate_logits[:, :, group_index * head_count:(group_index + 1) * head_count])
        blended = gate_values[0][..., None] * compressed_out + gate_values[1][..., None] * selected_out + gate_values[2][..., None] * windowed_out
        results.append(blended.reshape(STRETCH, head_count * DV))
    return jnp.concatenate(results, axis=1).astype(jnp.bfloat16)
```

```python
import functools
import math

import jax
import jax.numpy as jnp
from jax import lax
from jax.experimental import pallas as pl
from jax.experimental.pallas import tpu as pltpu
from jax.sharding import PartitionSpec as P

SBLK = 64
WINDOW = 512
XN, ZN = 4, 8
CN = XN * ZN
HEADS = 16
DK, DV = 192, 128
UNIT = 128
PACK = UNIT * 5 // 2
SPACK = SBLK * 5 // 2
NEAR = (0, 1, 7, 2)
FAR = (6, 3, 5, 4)
ROWS = 2048
CHUNK = 512
MESH = pl.DeviceIdType.MESH
LOW = -1e30
CEXP = math.log2(math.e) / math.sqrt(DK)
F32 = jnp.float32
BF16 = jnp.bfloat16


def pack_keys(k):
    n = k.shape[0]
    tail = k[:, 128:192]
    return k[:, :128], jnp.concatenate([tail[: n // 2], tail[n // 2 :]], axis=1)


def dot_t(a, b):
    return lax.dot_general(a, b, (((1,), (1,)), ((), ())), preferred_element_type=F32)


def body(
    asked,
    picks,
    cw,
    lengths,
    queries,
    sk,
    sv,
    ck,
    cv,
    gl,
    out,
    gat,
    send,
    recv,
    win,
    qs,
    acc,
    peak,
    mixed,
    gate,
    kt,
    vt,
    z_send,
    x_send,
    x2_send,
    d_send,
    g_recv,
    a_send,
    a_recv,
    w_send,
    w_recv,
    f_send,
    f_recv,
):
    ctx = lax.axis_index("ctx")
    p = lax.axis_index("pb")
    x = ctx // ZN
    z = lax.rem(ctx, ZN)
    flat = ctx * 2 + p
    other = 1 - p

    def at(dx, dz):
        return lax.rem(x + dx + XN, XN) * ZN + lax.rem(z + dz + ZN, ZN)

    def remote(src, dst, ssem, rsem, c, q):
        return pltpu.make_async_remote_copy(
            src_ref=src,
            dst_ref=dst,
            send_sem=ssem,
            recv_sem=rsem,
            device_id={"ctx": c, "pb": q},
            device_id_type=MESH,
        )

    barrier = pltpu.get_barrier_semaphore()

    def greet(i, carry):
        c = lax.rem(ctx + i // 2, CN)
        q = lax.rem(p + lax.rem(i, 2), 2)
        pl.semaphore_signal(barrier, inc=1, device_id={"ctx": c, "pb": q}, device_id_type=MESH)
        return carry

    lax.fori_loop(1, 2 * CN, greet, 0)

    k0, k1 = pack_keys(sk[...].astype(F32))
    win[4, 0:128, :] = k0.astype(BF16)
    win[4, 128:192, :] = k1.astype(BF16)
    win[4, 192:320, :] = sv[...]
    for k in range(1, 5):

        @pl.when(flat < k)
        def _():
            win[4 - k] = jnp.zeros((PACK, 128), BF16)

    b_at = p * UNIT + lax.broadcasted_iota(jnp.int32, (UNIT, 256), 0)
    j_at = lax.broadcasted_iota(jnp.int32, (UNIT, 256), 1)
    n_row = jnp.broadcast_to(lengths[...], (UNIT, 256)).astype(F32)
    starts = jnp.sum(jnp.where(j_at < b_at, n_row, 0.0), axis=1, keepdims=True)
    counts = jnp.sum(jnp.where(j_at == b_at, n_row, 0.0), axis=1, keepdims=True)
    spread = 1.0 / jnp.sqrt(counts)
    span = ck.shape[0] * SBLK
    step = 512
    total_k = jnp.zeros((UNIT, DK), F32)
    total_v = jnp.zeros((UNIT, DV), F32)
    for t in range(0, span, step):
        pos = (lax.broadcasted_iota(jnp.int32, (UNIT, step), 1) + t).astype(F32)
        away = pos - starts
        member = (away >= 0.0) & (away < counts)
        offs = jnp.sum(jnp.where(member, away, 0.0), axis=0, keepdims=True)
        weight = jnp.zeros((1, step), F32)
        for i in range(32):
            weight = jnp.where(offs == float(i), cw[0, i], weight)
        matrix = jnp.where(member, weight * spread, 0.0).astype(BF16)
        rows = ck[t // SBLK : (t + step) // SBLK].reshape(step, DK)
        vals = cv[t // SBLK : (t + step) // SBLK].reshape(step, DV)
        total_k += jnp.dot(matrix, rows, preferred_element_type=F32)
        total_v += jnp.dot(matrix, vals, preferred_element_type=F32)
    k0, k1 = pack_keys(total_k)
    gat[0, 0, p, 0:128, :] = k0.astype(BF16)
    gat[0, 0, p, 128:192, :] = k1.astype(BF16)
    gat[0, 0, p, 192:320, :] = total_v.astype(BF16)

    pl.semaphore_wait(barrier, 2 * CN - 1)

    def to_z(dz):
        return remote(
            gat.at[0, 0, p],
            gat.at[0, ZN - dz, p],
            z_send.at[dz],
            g_recv.at[0, ZN - dz, p],
            at(0, dz),
            p,
        )

    def to_x(zr, up):
        return remote(
            gat.at[0, zr, p],
            gat.at[3 if up else 1, zr, p],
            x_send.at[zr, 0 if up else 1],
            g_recv.at[3 if up else 1, zr, p],
            at(1 if up else -1, 0),
            p,
        )

    def to_x2(zr):
        near_row = 3 - 2 * p
        return remote(
            gat.at[near_row, zr, p],
            gat.at[2, zr, p],
            x2_send.at[zr],
            g_recv.at[2, zr, p],
            at(1 - 2 * p, 0),
            p,
        )

    def to_d(xr, zr):
        return remote(
            gat.at[xr, zr, p],
            gat.at[xr, zr, p],
            d_send.at[xr, zr],
            g_recv.at[xr, zr, p],
            ctx,
            other,
        )

    def arrive(xr, zr, q):
        remote(
            gat.at[xr, zr, q], gat.at[xr, zr, q], d_send.at[xr, zr], g_recv.at[xr, zr, q], ctx, other
        ).wait_recv()

    for dz in (1, 7, 2, 6, 3, 5, 4):
        to_z(dz).start()
    to_x(0, True).start()
    to_x(0, False).start()
    to_d(0, 0).start()

    def to_w(k):
        f = flat + k
        return remote(
            win.at[4], win.at[4 - k], w_send.at[k - 1], w_recv.at[k - 1], f // 2, lax.rem(f, 2)
        )

    for k in range(1, 5):

        @pl.when(flat + k < 2 * CN)
        def _():
            to_w(k).start()

    def store_block(ref, at_index, number):
        a0, a1 = pack_keys(ck[number].astype(F32))
        ref[at_index, 0:64, :] = a0.astype(BF16)
        ref[at_index, 64:96, :] = a1.astype(BF16)
        ref[at_index, 96:160, :] = cv[number]

    def first_fixed(i):
        return remote(
            recv.at[64],
            recv.at[64],
            f_send.at[i],
            f_recv.at[0],
            lax.rem(ctx + i, CN),
            p,
        )

    def last_fixed(i):
        return remote(
            recv.at[pl.ds(65, 2)],
            recv.at[pl.ds(65, 2)],
            f_send.at[i],
            f_recv.at[1],
            lax.rem(ctx + i, CN),
            p,
        )

    def start_all(make):
        def one(i, carry):
            make(i).start()
            return carry

        lax.fori_loop(1, CN, one, 0)

    def sent_all(make):
        def one(i, carry):
            make(i).wait_send()
            return carry

        lax.fori_loop(1, CN, one, 0)

    @pl.when(ctx == 0)
    def _():
        store_block(recv, 64, 0)
        start_all(first_fixed)

    @pl.when(ctx == CN - 1)
    def _():
        store_block(recv, 65, SBLK - 2)
        store_block(recv, 66, SBLK - 1)
        start_all(last_fixed)

    def to_a(i):
        dx, dz = i // ZN, lax.rem(i, ZN)
        back = lax.rem(XN - dx, XN) * ZN + lax.rem(ZN - dz, ZN)
        return remote(
            send.at[pl.ds(2 * i, 2)],
            recv.at[pl.ds(2 * back, 2)],
            a_send.at[i],
            a_recv.at[back],
            at(dx, dz),
            p,
        )

    for j in range(2):
        store_block(recv, j, asked[ctx, j])

    def fill(i, carry):
        c = at(i // ZN, lax.rem(i, ZN))
        for j in range(2):
            store_block(send, 2 * i + j, asked[c, j])
        to_a(i).start()
        return carry

    lax.fori_loop(1, CN, fill, 0)

    lane = lax.broadcasted_iota(jnp.int32, (UNIT, 256), 1)
    gates = [jax.nn.sigmoid(gl[i]) for i in range(3)]
    for pair in range(HEADS // 2):
        both = queries[:, pair * 384 : (pair + 1) * 384].astype(F32)
        first = jnp.where(lane < DK, both[:, 0:256], 0.0).astype(BF16)
        second = jnp.where(lane < DK, pltpu.roll(both[:, 128:384], 192, 1), 0.0).astype(BF16)
        for h, rows in ((2 * pair, first), (2 * pair + 1, second)):
            for b in range(2):
                base = b * 1024 + h * 64
                qs[base : base + 64, :] = rows[b * 64 : b * 64 + 64]
                for i in range(3):
                    gate[i, base : base + 64, :] = jnp.broadcast_to(
                        gates[i][b * 64 : b * 64 + 64, h : h + 1], (64, 128)
                    )
    vt[:, 128:256] = jnp.ones((1024, 128), BF16)

    def unpack(ref_at, n, base):
        half = ref_at[n : n + n // 2, :]
        kt[base : base + n, 0:128] = ref_at[0:n, :]
        kt[base : base + n // 2, 128:256] = half
        kt[base + n // 2 : base + n, 128:256] = pltpu.roll(half.astype(F32), 64, 1).astype(BF16)
        vt[base : base + n, 0:128] = ref_at[n + n // 2 : 2 * n + n // 2, :]

    for k in range(1, 5):

        @pl.when(flat >= k)
        def _():
            remote(
                win.at[4 - k], win.at[4 - k], w_send.at[k - 1], w_recv.at[k - 1], ctx, other
            ).wait_recv()

    for k in range(5):
        unpack(win.at[k], UNIT, k * UNIT)

    def window_chunk(r, carry):
        rows = pl.ds(pl.multiple_of(r * CHUNK, CHUNK), CHUNK)
        width = WINDOW + UNIT
        s = dot_t(qs[rows, :], kt[0:width, :])
        i_at = lax.rem(lax.broadcasted_iota(jnp.int32, (CHUNK, width), 0), 64)
        j_at = lax.broadcasted_iota(jnp.int32, (CHUNK, width), 1)
        dist = WINDOW + (r // 2) * 64 + i_at - j_at
        allowed = (dist >= 0) & (dist < WINDOW) & (j_at >= WINDOW - flat * UNIT)
        s = jnp.where(allowed, s * CEXP, LOW)
        e = jnp.exp2(s - jnp.max(s, axis=1, keepdims=True)).astype(BF16)
        o = jnp.dot(e, vt[0:width, :], preferred_element_type=F32)
        mixed[rows, :] = gate[2, rows, :] * (o[:, 0:128] / o[:, 128:256])
        peak[rows, :] = jnp.full((CHUNK, 128), LOW, F32)
        acc[rows, :] = jnp.zeros((CHUNK, 256), F32)
        return carry

    lax.fori_loop(0, ROWS // CHUNK, window_chunk, 0)

    def tile(xr, zs):
        for n, zr in enumerate(zs):
            for q in range(2):
                unpack(gat.at[xr, zr, q], UNIT, n * 256 + q * UNIT)

        def chunk(r, carry):
            rows = pl.ds(pl.multiple_of(r * CHUNK, CHUNK), CHUNK)
            s = dot_t(qs[rows, :], kt[...])
            before = peak[rows, :]
            top = jnp.maximum(before, jnp.max(s, axis=1, keepdims=True) * CEXP)
            e = jnp.exp2(s * CEXP - top[:, 0:1]).astype(BF16)
            factor = jnp.exp2(before - top)
            o = jnp.dot(e, vt[...], preferred_element_type=F32)
            acc[rows, 0:128] = acc[rows, 0:128] * factor + o[:, 0:128]
            acc[rows, 128:256] = acc[rows, 128:256] * factor + o[:, 128:256]
            peak[rows, :] = top
            return carry

        lax.fori_loop(0, ROWS // CHUNK, chunk, 0)

    for zs in (NEAR, FAR):
        for zr in zs:
            if zr:
                arrive(0, zr, p)
                to_x(zr, True).start()
                to_x(zr, False).start()
                to_d(0, zr).start()
        for zr in zs:
            arrive(0, zr, other)
        tile(0, zs)
    for zs in (NEAR, FAR):
        for zr in zs:
            arrive(3, zr, p)
            to_d(3, zr).start()
            arrive(1, zr, p)
            to_d(1, zr).start()
            to_x2(zr).start()
        for xr in (3, 1):
            for zr in zs:
                arrive(xr, zr, other)
            tile(xr, zs)
    for zs in (NEAR, FAR):
        for zr in zs:
            arrive(2, zr, p)
            to_d(2, zr).start()
        for zr in zs:
            arrive(2, zr, other)
        tile(2, zs)

    def settle(r, carry):
        rows = pl.ds(pl.multiple_of(r * CHUNK, CHUNK), CHUNK)
        mixed[rows, :] += gate[0, rows, :] * (acc[rows, 0:128] / acc[rows, 128:256])
        return carry

    lax.fori_loop(0, ROWS // CHUNK, settle, 0)

    def got_a(i, carry):
        remote(
            send.at[pl.ds(2 * i, 2)], recv.at[pl.ds(2 * i, 2)], a_send.at[i], a_recv.at[i], ctx, other
        ).wait_recv()
        return carry

    lax.fori_loop(1, CN, got_a, 0)

    @pl.when(ctx != 0)
    def _():
        first_fixed(1).wait_recv()

    @pl.when(ctx != CN - 1)
    def _():
        last_fixed(1).wait_recv()

    for b in range(2):
        for n in range(16):
            number = 64 + n if n < 3 else picks[b, n - 3]
            block = recv[number]
            kt[n * 64 : n * 64 + 64, 0:128] = block[0:64]
            kt[n * 64 : n * 64 + 32, 128:256] = block[64:96]
            kt[n * 64 + 32 : n * 64 + 64, 128:256] = pltpu.roll(
                block[64:96].astype(F32), 64, 1
            ).astype(BF16)
            vt[n * 64 : n * 64 + 64, 0:128] = block[96:160]
        for r in range(1024 // CHUNK):
            base = b * 1024 + r * CHUNK
            rows = pl.ds(base, CHUNK)
            s = dot_t(qs[rows, :], kt[...]) * CEXP
            e = jnp.exp2(s - jnp.max(s, axis=1, keepdims=True)).astype(BF16)
            o = jnp.dot(e, vt[...], preferred_element_type=F32)
            done = mixed[rows, :] + gate[1, rows, :] * (o[:, 0:128] / o[:, 128:256])
            for h in range(CHUNK // 64):
                head = r * (CHUNK // 64) + h
                out[b * 64 : b * 64 + 64, head * 128 : head * 128 + 128] = done[
                    h * 64 : h * 64 + 64
                ].astype(BF16)

    for dz in range(1, ZN):
        to_z(dz).wait_send()
    for zr in range(ZN):
        to_x(zr, True).wait_send()
        to_x(zr, False).wait_send()
        to_x2(zr).wait_send()
        for xr in range(XN):
            to_d(xr, zr).wait_send()
    for k in range(1, 5):

        @pl.when(flat + k < 2 * CN)
        def _():
            to_w(k).wait_send()

    sent_all(to_a)

    @pl.when(ctx == 0)
    def _():
        sent_all(first_fixed)

    @pl.when(ctx == CN - 1)
    def _():
        sent_all(last_fixed)


def wanted(listed):
    ids = listed.reshape(-1)
    owner = ids // SBLK
    place = jnp.arange(ids.shape[0], dtype=jnp.int32)
    before = (owner[None, :] == owner[:, None]) & (place[None, :] < place[:, None])
    rank = jnp.sum(before.astype(jnp.int32), axis=1)
    slots = owner * 2 + rank
    cells = jnp.arange(CN * 2, dtype=jnp.int32)
    table = jnp.sum(jnp.where(slots[:, None] == cells[None, :], (ids % SBLK)[:, None], 0), axis=0)
    return owner, rank, table.reshape(CN, 2)


def on_device(queries, sk, sv, pk, cv, lengths, cw, selections, gl):
    listed = selections[:, 0, :]
    owner, rank, table = wanted(listed)
    asked = lax.all_to_all(table, "ctx", split_axis=0, concat_axis=0, tiled=True)
    ctx = lax.axis_index("ctx")
    rel = ((owner // ZN - ctx // ZN) % XN) * ZN + (owner % ZN - ctx % ZN) % ZN
    picks = (rel * 2 + rank).reshape(listed.shape)
    blocks = pk.shape[0] // SBLK
    vmem = pl.BlockSpec(memory_space=pltpu.VMEM)
    smem = pl.BlockSpec(memory_space=pltpu.SMEM)
    dma = pltpu.SemaphoreType.DMA
    return pl.pallas_call(
        body,
        name="attend",
        out_shape=jax.ShapeDtypeStruct((queries.shape[0], HEADS * DV), BF16),
        in_specs=[smem] * 3 + [vmem] * 7,
        out_specs=vmem,
        scratch_shapes=[
            pltpu.VMEM((XN, ZN, 2, PACK, 128), BF16),
            pltpu.VMEM((2 * CN, SPACK, 128), BF16),
            pltpu.VMEM((2 * CN + 3, SPACK, 128), BF16),
            pltpu.VMEM((5, PACK, 128), BF16),
            pltpu.VMEM((ROWS, 256), BF16),
            pltpu.VMEM((ROWS, 256), F32),
            pltpu.VMEM((ROWS, 128), F32),
            pltpu.VMEM((ROWS, 128), F32),
            pltpu.VMEM((3, ROWS, 128), F32),
            pltpu.VMEM((1024, 256), BF16),
            pltpu.VMEM((1024, 256), BF16),
            dma((ZN,)),
            dma((ZN, 2)),
            dma((ZN,)),
            dma((XN, ZN)),
            dma((XN, ZN, 2)),
            dma((CN,)),
            dma((CN,)),
            dma((4,)),
            dma((4,)),
            dma((CN,)),
            dma((2,)),
        ],
        compiler_params=pltpu.CompilerParams(
            collective_id=0, has_side_effects=True, vmem_limit_bytes=60 * 1024 * 1024
        ),
    )(
        asked,
        picks,
        cw,
        lengths,
        queries,
        sk,
        sv,
        pk.reshape(blocks, SBLK, DK),
        cv.reshape(blocks, SBLK, DV),
        gl,
    )


def solution(mesh):
    placed = (
        P(("ctx", "pb"), "ga"),
        P(("ctx", "pb"), "ga"),
        P(("ctx", "pb"), "ga"),
        P("ctx", "ga"),
        P("ctx", "ga"),
        P("ctx", None),
        P("ga", None),
        P(("ctx", "pb"), "ga", None),
        P(None, ("ctx", "pb"), "ga"),
    )
    return jax.shard_map(
        on_device, mesh=mesh, in_specs=placed, out_specs=P(("ctx", "pb"), "ga"), check_vma=False
    )
```

```python
import functools
import math

import jax
import jax.numpy as jnp
from jax import lax
from jax.experimental import pallas as pl
from jax.experimental.pallas import tpu as pltpu
from jax.sharding import PartitionSpec as P

SBLK = 64
WINDOW = 512
XN, ZN = 4, 8
CN = XN * ZN
HEADS = 16
DK, DV = 192, 128
UNIT = 128
PACK = UNIT * 5 // 2
SPACK = SBLK * 5 // 2
ZSET = ((0, 1, 7, 2), (6, 3, 5, 4))
ORDER = ((0, 0), (0, 1), (3, 0), (1, 0), (3, 1), (1, 1), (2, 0), (2, 1))
PACE = (3, 3, 4, 4, 4, 4, 4, 5)
ROWS = 2048
CHUNK = 512
MESH = pl.DeviceIdType.MESH
LOW = -1e30
CEXP = math.log2(math.e) / math.sqrt(DK)
F32 = jnp.float32
BF16 = jnp.bfloat16


def pack_keys(k):
    n = k.shape[0]
    tail = k[:, 128:192]
    return k[:, :128], jnp.concatenate([tail[: n // 2], tail[n // 2 :]], axis=1)


def dot_t(a, b):
    return lax.dot_general(a, b, (((1,), (1,)), ((), ())), preferred_element_type=F32)


def slot(xr, zr):
    far = 0 if zr in ZSET[0] else 1
    return ORDER.index((xr, far)), ZSET[far].index(zr)


def body(
    cw,
    sel_s,
    sel,
    lengths,
    queries,
    sk,
    sv,
    ck,
    cv,
    gl,
    out,
    gat,
    send,
    recv,
    win,
    mine,
    reqs,
    offs,
    asked,
    qs,
    acc,
    peak,
    mixed,
    gate,
    kt,
    vt,
    vr,
    sbuf,
    z_send,
    x_send,
    x2_send,
    d_send,
    g_recv,
    a_send,
    a_recv,
    w_send,
    wd_send,
    w_recv,
    f_send,
    f_recv,
    q_send,
    q_recv,
    l_sem,
):
    ctx = lax.axis_index("ctx")
    p = lax.axis_index("pb")
    x = ctx // ZN
    z = lax.rem(ctx, ZN)
    flat = ctx * 2 + p
    other = 1 - p

    def at(dx, dz):
        return lax.rem(x + dx + XN, XN) * ZN + lax.rem(z + dz + ZN, ZN)

    def remote(src, dst, ssem, rsem, c, q):
        return pltpu.make_async_remote_copy(
            src_ref=src,
            dst_ref=dst,
            send_sem=ssem,
            recv_sem=rsem,
            device_id={"ctx": c, "pb": q},
            device_id_type=MESH,
        )

    barrier = pltpu.get_barrier_semaphore()

    def greet(i, carry):
        c = lax.rem(ctx + i // 2, CN)
        q = lax.rem(p + lax.rem(i, 2), 2)
        pl.semaphore_signal(barrier, inc=1, device_id={"ctx": c, "pb": q}, device_id_type=MESH)
        return carry

    lax.fori_loop(1, 2 * CN, greet, 0)

    mine[...] = jnp.full((2, 1, 128), -1, jnp.int32)
    for b in range(2):
        mine[b, :, 0:13] = sel[b]
    reqs[0] = jnp.full((2, 1, 128), -1, jnp.int32)
    for b in range(2):
        reqs[0, b, :, 0:13] = sel[b]
    k0, k1 = pack_keys(sk[...].astype(F32))
    win[0, p, 0:128, :] = k0.astype(BF16)
    win[0, p, 128:192, :] = k1.astype(BF16)
    win[0, p, 192:320, :] = sv[...].astype(F32).T.astype(BF16)
    for k in range(1, 3):

        @pl.when(ctx < k)
        def _():
            win[k] = jnp.zeros((2, PACK, 128), BF16)

    b_at = p * UNIT + lax.broadcasted_iota(jnp.int32, (UNIT, 256), 0)
    j_at = lax.broadcasted_iota(jnp.int32, (UNIT, 256), 1)
    n_row = jnp.broadcast_to(lengths[...], (UNIT, 256)).astype(F32)
    starts = jnp.sum(jnp.where(j_at < b_at, n_row, 0.0), axis=1, keepdims=True)
    counts = jnp.sum(jnp.where(j_at == b_at, n_row, 0.0), axis=1, keepdims=True)
    spread = 1.0 / jnp.sqrt(counts)
    span = ck.shape[0] * SBLK
    step = 512
    total_k = jnp.zeros((UNIT, DK), F32)
    total_v = jnp.zeros((UNIT, DV), F32)
    for t in range(0, span, step):
        pos = (lax.broadcasted_iota(jnp.int32, (UNIT, step), 1) + t).astype(F32)
        away = pos - starts
        member = (away >= 0.0) & (away < counts)
        off = jnp.sum(jnp.where(member, away, 0.0), axis=0, keepdims=True)
        weight = jnp.zeros((1, step), F32)
        for i in range(32):
            weight = jnp.where(off == float(i), cw[0, i], weight)
        matrix = jnp.where(member, weight * spread, 0.0).astype(BF16)
        rows = ck[t // SBLK : (t + step) // SBLK].reshape(step, DK)
        vals = cv[t // SBLK : (t + step) // SBLK].reshape(step, DV)
        total_k += jnp.dot(matrix, rows, preferred_element_type=F32)
        total_v += jnp.dot(matrix, vals, preferred_element_type=F32)
    k0, k1 = pack_keys(total_k)
    gat[0, 0, p, 0:128, :] = k0.astype(BF16)
    gat[0, 0, p, 128:192, :] = k1.astype(BF16)
    gat[0, 0, p, 192:320, :] = total_v.T.astype(BF16)

    pl.semaphore_wait(barrier, 2 * CN - 1)

    def to_q(i):
        dx, dz = i // ZN, lax.rem(i, ZN)
        back = lax.rem(XN - dx, XN) * ZN + lax.rem(ZN - dz, ZN)
        return remote(mine, reqs.at[back], q_send.at[i], q_recv.at[back], at(dx, dz), p)

    def got_q(i, carry):
        remote(mine, reqs.at[i], q_send.at[i], q_recv.at[i], ctx, other).wait_recv()
        return carry

    def start_all(make):
        def one(i, carry):
            make(i).start()
            return carry

        lax.fori_loop(1, CN, one, 0)

    def sent_all(make):
        def one(i, carry):
            make(i).wait_send()
            return carry

        lax.fori_loop(1, CN, one, 0)

    start_all(to_q)

    def g_at(xr, zr, q):
        t, n = slot(xr, zr)
        return gat.at[t, n, q]

    def g_sem(xr, zr, q):
        t, n = slot(xr, zr)
        return g_recv.at[t, n, q]

    def to_z(zr, up):
        return remote(
            g_at(0, zr, p),
            g_at(0, (zr + (7 if up else 1)) % ZN, p),
            z_send.at[zr, 0 if up else 1],
            g_sem(0, (zr + (7 if up else 1)) % ZN, p),
            at(0, 1 if up else -1),
            p,
        )

    def to_x(zr, up):
        return remote(
            g_at(0, zr, p),
            g_at(3 if up else 1, zr, p),
            x_send.at[zr, 0 if up else 1],
            g_sem(3 if up else 1, zr, p),
            at(1 if up else -1, 0),
            p,
        )

    def to_x2(zr):
        t3, n = slot(3, zr)
        t1, _ = slot(1, zr)
        return remote(
            gat.at[t3 + p * (t1 - t3), n, p],
            g_at(2, zr, p),
            x2_send.at[zr],
            g_sem(2, zr, p),
            at(1 - 2 * p, 0),
            p,
        )

    def to_d(xr, zr):
        return remote(
            g_at(xr, zr, p), g_at(xr, zr, p), d_send.at[xr, zr], g_sem(xr, zr, p), ctx, other
        )

    def arrive(xr, zr, q):
        remote(
            g_at(xr, zr, q), g_at(xr, zr, q), d_send.at[xr, zr], g_sem(xr, zr, q), ctx, other
        ).wait_recv()

    def spread_on(zr):
        if zr in (0, 7, 6):
            to_z(zr, True).start()
        if zr in (0, 1, 2):
            to_z(zr, False).start()
        if zr == 5:

            @pl.when(p == 0)
            def _():
                to_z(5, True).start()

        if zr == 3:

            @pl.when(p == 1)
            def _():
                to_z(3, False).start()

        to_x(zr, True).start()
        to_x(zr, False).start()
        to_d(0, zr).start()

    spread_on(0)

    def to_w(k):
        return remote(
            win.at[k, p], win.at[k + 1, p], w_send.at[k], w_recv.at[k + 1, p], lax.rem(ctx + 1, CN), p
        )

    def to_wd(k):
        return remote(win.at[k, p], win.at[k, p], wd_send.at[k], w_recv.at[k, p], ctx, other)

    def got_w(k, q):
        remote(win.at[k, q], win.at[k, q], wd_send.at[k], w_recv.at[k, q], ctx, other).wait_recv()

    @pl.when(ctx + 1 < CN)
    def _():
        to_w(0).start()

    to_wd(0).start()

    def store_block(ref, at_index, number):
        a0, a1 = pack_keys(ck[number].astype(F32))
        ref[at_index, 0:64, :] = a0.astype(BF16)
        ref[at_index, 64:96, :] = a1.astype(BF16)
        ref[at_index, 96:160, :] = cv[number]

    def first_fixed(i):
        return remote(
            recv.at[64], recv.at[64], f_send.at[i], f_recv.at[0], lax.rem(ctx + i, CN), p
        )

    def last_fixed(i):
        return remote(
            recv.at[pl.ds(65, 2)],
            recv.at[pl.ds(65, 2)],
            f_send.at[i],
            f_recv.at[1],
            lax.rem(ctx + i, CN),
            p,
        )

    @pl.when(ctx == 0)
    def _():
        store_block(recv, 64, 0)
        start_all(first_fixed)

    @pl.when(ctx == CN - 1)
    def _():
        store_block(recv, 65, SBLK - 2)
        store_block(recv, 66, SBLK - 1)
        start_all(last_fixed)

    lane = lax.broadcasted_iota(jnp.int32, (UNIT, 256), 1)
    for pair in range(HEADS // 2):
        both = queries[:, pair * 384 : (pair + 1) * 384].astype(F32)
        first = jnp.where(lane < DK, both[:, 0:256], 0.0).astype(BF16)
        second = jnp.where(lane < DK, pltpu.roll(both[:, 128:384], 192, 1), 0.0).astype(BF16)
        for h, rows in ((2 * pair, first), (2 * pair + 1, second)):
            for b in range(2):
                base = b * 1024 + h * 64
                qs[base : base + 64, :] = rows[b * 64 : b * 64 + 64]

    lfn = pltpu.make_async_copy(offs, asked, l_sem)
    lax.fori_loop(1, CN, got_q, 0)
    big = 1 << 20
    lanes = lax.broadcasted_iota(jnp.int32, (CN, 1, 128), 2)
    keys = []
    for b in range(2):
        ids = reqs[:, b]
        here = (ids >= ctx * SBLK) & (ids < (ctx + 1) * SBLK)
        keys.append(jnp.where(here, b * 8192 + lanes * SBLK + ids - ctx * SBLK, big))
    one = jnp.min(jnp.minimum(keys[0], keys[1]), axis=2, keepdims=True)
    rest = [jnp.where(k > one, k, big) for k in keys]
    two = jnp.min(jnp.minimum(rest[0], rest[1]), axis=2, keepdims=True)
    offs[...] = jnp.where(lanes == 0, one, two) & (SBLK - 1)
    lfn.start()

    lane = lax.broadcasted_iota(jnp.int32, (8, 128), 1)
    for i in range(3):
        g = jax.nn.sigmoid(gl[i])
        turned = pltpu.roll(g, 64, 1)
        for b in range(2):
            for h in range(0, HEADS, 2):
                low = (g, turned)[b][h : h + 1]
                high = (turned, g)[b][h + 1 : h + 2]
                c, n = b * 2 + h // 8, (h % 8) * 64
                gate[i, c, :, n : n + 128] = jnp.where(lane < 64, low, high)
    vt[128:144, :] = jnp.ones((16, 1024), BF16)

    def unpack_keys(ref_at, n, base):
        half = ref_at[n : n + n // 2, :]
        kt[base : base + n, 0:128] = ref_at[0:n, :]
        kt[base : base + n // 2, 128:256] = half
        kt[base + n // 2 : base + n, 128:256] = pltpu.roll(half.astype(F32), 64, 1).astype(BF16)

    def unpack(ref_at, base):
        unpack_keys(ref_at, UNIT, base)
        vt[0:128, base : base + UNIT] = ref_at[192:320, :]

    lfn.wait()

    def to_a(i):
        dx, dz = i // ZN, lax.rem(i, ZN)
        back = lax.rem(XN - dx, XN) * ZN + lax.rem(ZN - dz, ZN)
        return remote(
            send.at[pl.ds(2 * i, 2)],
            recv.at[pl.ds(2 * back, 2)],
            a_send.at[i],
            a_recv.at[back],
            at(dx, dz),
            p,
        )

    for j in range(2):
        store_block(recv, j, asked[0, 0, j])

    def fill(n, carry):
        i = lax.rem(n * 5, CN)
        for j in range(2):
            store_block(send, 2 * i + j, asked[i, 0, j])
        to_a(i).start()
        return carry

    def listed(stage):
        lax.fori_loop(1 + sum(PACE[:stage]), 1 + sum(PACE[: stage + 1]), fill, 0)

    listed(0)

    for zr in (1, 7):
        arrive(0, zr, p)
        spread_on(zr)

    @pl.when(ctx >= 1)
    def _():
        got_w(1, p)
        to_wd(1).start()

        @pl.when(ctx + 1 < CN)
        def _():
            to_w(1).start()

    listed(1)

    for zr in (2, 6):
        arrive(0, zr, p)
        spread_on(zr)

    @pl.when(ctx >= 2)
    def _():
        got_w(2, p)
        to_wd(2).start()

    got_w(0, other)
    for k in (1, 2):

        @pl.when(ctx >= k)
        def _():
            got_w(k, other)

    for k in range(5):
        unpack(win.at[2 - (p + k) // 2, lax.rem(p + k, 2)], k * UNIT)
    near = WINDOW + UNIT

    def scores(c, width):
        return dot_t(kt[0:width, :], qs[c * CHUNK : (c + 1) * CHUNK, :])

    def mix(e, width):
        return jnp.dot(vt[:, 0:width], e, preferred_element_type=F32)

    sbuf[0, 0:near, :] = scores(0, near)
    for c in range(4):
        if c < 3:
            sbuf[(c + 1) % 2, 0:near, :] = scores(c + 1, near)
        i_at = lax.broadcasted_iota(jnp.int32, (near, CHUNK), 1) & 63
        j_at = lax.broadcasted_iota(jnp.int32, (near, CHUNK), 0)
        dist = WINDOW + (c // 2) * 64 + i_at - j_at
        allowed = (dist >= 0) & (dist < WINDOW) & (j_at >= WINDOW - flat * UNIT)
        sc = jnp.where(allowed, sbuf[c % 2, 0:near, :] * CEXP, LOW)
        e = jnp.exp2(sc - jnp.max(sc, axis=0, keepdims=True)).astype(BF16)
        o = mix(e, near)
        mixed[c] = o[0:128] * (gate[2, c, 0:1] / o[128:129])
        peak[c] = jnp.full((8, CHUNK), LOW, F32)
        acc[c] = jnp.zeros((144, CHUNK), F32)

    def stage(t):
        if t == 0:
            for zr in (3, 5):
                arrive(0, zr, p)
                spread_on(zr)
            need = [(0, zr) for zr in ZSET[0]]
        elif t == 1:
            arrive(0, 4, p)
            spread_on(4)
            need = [(0, zr) for zr in ZSET[1]]
        else:
            xr, far = ORDER[t]
            need = [(xr, zr) for zr in ZSET[far]]
            if xr == 3:
                for zr in ZSET[far]:
                    arrive(3, zr, p)
                    to_d(3, zr).start()
                    arrive(1, zr, p)
                    to_d(1, zr).start()
                    to_x2(zr).start()
            elif xr == 2:
                for zr in ZSET[far]:
                    arrive(2, zr, p)
                    to_d(2, zr).start()
        if t < 6:
            listed(t + 2)
        for xr, zr in need:
            arrive(xr, zr, other)

    def tile(t, carry):
        for k in range(8):

            @pl.when(t == k)
            def _():
                stage(k)

        for n in range(4):
            for q in range(2):
                unpack(gat.at[t, n, q], n * 256 + q * UNIT)
        sbuf[0] = scores(0, 1024)
        for c in range(4):
            if c < 3:
                sbuf[(c + 1) % 2] = scores(c + 1, 1024)
            sc = sbuf[c % 2]
            before = peak[c]
            top = jnp.maximum(before, jnp.max(sc, axis=0, keepdims=True) * CEXP)
            e = jnp.exp2(sc * CEXP - top[0:1]).astype(BF16)
            factor = jnp.exp2(before - top)[0:1]
            acc[c] = acc[c] * factor + mix(e, 1024)
            peak[c] = top
        return carry

    lax.fori_loop(0, 8, tile, 0)

    for c in range(4):
        mixed[c] += acc[c, 0:128] * (gate[0, c, 0:1] / acc[c, 128:129])

    def got_a(i, carry):
        remote(
            send.at[pl.ds(2 * i, 2)], recv.at[pl.ds(2 * i, 2)], a_send.at[i], a_recv.at[i], ctx, other
        ).wait_recv()
        return carry

    lax.fori_loop(1, CN, got_a, 0)

    @pl.when(ctx != 0)
    def _():
        first_fixed(1).wait_recv()

    @pl.when(ctx != CN - 1)
    def _():
        last_fixed(1).wait_recv()

    ids = [sel_s[b, 0, n] for b in range(2) for n in range(13)]
    owner = [i // SBLK for i in ids]
    picks = []
    for n, own in enumerate(owner):
        rank = 0
        for m in range(n):
            rank = rank + jnp.where(owner[m] == own, 1, 0)
        ox, oz = own // ZN, own % ZN
        rel = ((ox + XN - x) % XN) * ZN + (oz + ZN - z) % ZN
        picks.append(rel * 2 + jnp.minimum(rank, 1))
    for b in range(2):
        for n in range(16):
            number = 64 + n if n < 3 else picks[b * 13 + n - 3]
            block = recv[number]
            unpack_keys(block, SBLK, n * SBLK)
            vr[n * 64 : n * 64 + 64, :] = block[96:160]
        vt[0:128, :] = vr[...].T
        sbuf[0] = scores(2 * b, 1024)
        for r in range(2):
            if r == 0:
                sbuf[1] = scores(2 * b + 1, 1024)
            c = 2 * b + r
            sc = sbuf[r] * CEXP
            e = jnp.exp2(sc - jnp.max(sc, axis=0, keepdims=True)).astype(BF16)
            o = mix(e, 1024)
            done = (mixed[c] + o[0:128] * (gate[1, c, 0:1] / o[128:129])).T
            for h in range(CHUNK // 64):
                head = r * (CHUNK // 64) + h
                out[b * 64 : b * 64 + 64, head * 128 : head * 128 + 128] = done[
                    h * 64 : h * 64 + 64
                ].astype(BF16)

    for zr in (0, 7, 6):
        to_z(zr, True).wait_send()
    for zr in (0, 1, 2):
        to_z(zr, False).wait_send()

    @pl.when(p == 0)
    def _():
        to_z(5, True).wait_send()

    @pl.when(p == 1)
    def _():
        to_z(3, False).wait_send()

    for zr in range(ZN):
        to_x(zr, True).wait_send()
        to_x(zr, False).wait_send()
        to_x2(zr).wait_send()
        for xr in range(XN):
            to_d(xr, zr).wait_send()
    to_wd(0).wait_send()

    @pl.when(ctx + 1 < CN)
    def _():
        to_w(0).wait_send()

    @pl.when(ctx >= 1)
    def _():
        to_wd(1).wait_send()

        @pl.when(ctx + 1 < CN)
        def _():
            to_w(1).wait_send()

    @pl.when(ctx >= 2)
    def _():
        to_wd(2).wait_send()

    sent_all(to_q)
    sent_all(to_a)

    @pl.when(ctx == 0)
    def _():
        sent_all(first_fixed)

    @pl.when(ctx == CN - 1)
    def _():
        sent_all(last_fixed)


def on_device(queries, sk, sv, pk, cv, lengths, cw, selections, gl):
    blocks = pk.shape[0] // SBLK
    vmem = pl.BlockSpec(memory_space=pltpu.VMEM)
    smem = pl.BlockSpec(memory_space=pltpu.SMEM)
    dma = pltpu.SemaphoreType.DMA
    return pl.pallas_call(
        body,
        name="attend",
        out_shape=jax.ShapeDtypeStruct((queries.shape[0], HEADS * DV), BF16),
        in_specs=[smem] * 2 + [vmem] * 8,
        out_specs=vmem,
        scratch_shapes=[
            pltpu.VMEM((8, 4, 2, PACK, 128), BF16),
            pltpu.VMEM((2 * CN, SPACK, 128), BF16),
            pltpu.VMEM((2 * CN + 3, SPACK, 128), BF16),
            pltpu.VMEM((3, 2, PACK, 128), BF16),
            pltpu.VMEM((2, 1, 128), jnp.int32),
            pltpu.VMEM((CN, 2, 1, 128), jnp.int32),
            pltpu.VMEM((CN, 1, 128), jnp.int32),
            pltpu.SMEM((CN, 1, 128), jnp.int32),
            pltpu.VMEM((ROWS, 256), BF16),
            pltpu.VMEM((4, 144, CHUNK), F32),
            pltpu.VMEM((4, 8, CHUNK), F32),
            pltpu.VMEM((4, 128, CHUNK), F32),
            pltpu.VMEM((3, 4, 8, CHUNK), F32),
            pltpu.VMEM((1024, 256), BF16),
            pltpu.VMEM((144, 1024), BF16),
            pltpu.VMEM((1024, 128), BF16),
            pltpu.VMEM((2, 1024, CHUNK), F32),
            dma((ZN, 2)),
            dma((ZN, 2)),
            dma((ZN,)),
            dma((XN, ZN)),
            dma((8, 4, 2)),
            dma((CN,)),
            dma((CN,)),
            dma((2,)),
            dma((3,)),
            dma((3, 2)),
            dma((CN,)),
            dma((2,)),
            dma((CN,)),
            dma((CN,)),
            dma(()),
        ],
        compiler_params=pltpu.CompilerParams(
            collective_id=0, has_side_effects=True, vmem_limit_bytes=60 * 1024 * 1024
        ),
    )(
        cw,
        selections,
        selections,
        lengths,
        queries,
        sk,
        sv,
        pk.reshape(blocks, SBLK, DK),
        cv.reshape(blocks, SBLK, DV),
        jnp.transpose(gl, (0, 2, 1)),
    )


def solution(mesh):
    placed = (
        P(("ctx", "pb"), "ga"),
        P(("ctx", "pb"), "ga"),
        P(("ctx", "pb"), "ga"),
        P("ctx", "ga"),
        P("ctx", "ga"),
        P("ctx", None),
        P("ga", None),
        P(("ctx", "pb"), "ga", None),
        P(None, ("ctx", "pb"), "ga"),
    )
    return jax.shard_map(
        on_device, mesh=mesh, in_specs=placed, out_specs=P(("ctx", "pb"), "ga"), check_vma=False
    )
```

```python
import functools
import math

import jax
import jax.numpy as jnp
from jax import lax
from jax.experimental import pallas as pl
from jax.experimental.pallas import tpu as pltpu
from jax.sharding import PartitionSpec as P

SBLK = 64
WINDOW = 512
XN, ZN = 4, 8
CN = XN * ZN
HEADS = 16
DK, DV = 192, 128
UNIT = 128
PACK = UNIT * 5 // 2
SPACK = SBLK * 5 // 2
ZSET = ((0, 1, 7, 2), (6, 3, 5, 4))
ORDER = ((0, 0), (0, 1), (3, 0), (1, 0), (3, 1), (1, 1), (2, 0), (2, 1))
PACE = (5, 5, 6, 6, 6, 3, 0, 0)
ORIGIN = ((0, 0), (XN - 1, ZN - 1))
ROWS = 2048
CHUNK = 512
MESH = pl.DeviceIdType.MESH
LOW = -1e30
CEXP = math.log2(math.e) / math.sqrt(DK)
F32 = jnp.float32
BF16 = jnp.bfloat16


def pack_keys(k):
    n = k.shape[0]
    tail = k[:, 128:192]
    return k[:, :128], jnp.concatenate([tail[: n // 2], tail[n // 2 :]], axis=1)


def dot_t(a, b):
    return lax.dot_general(a, b, (((1,), (1,)), ((), ())), preferred_element_type=F32)


def slot(xr, zr):
    far = 0 if zr in ZSET[0] else 1
    return ORDER.index((xr, far)), ZSET[far].index(zr)


def body(
    cw,
    sel_s,
    sel,
    lengths,
    queries,
    sk,
    sv,
    ck,
    cv,
    gl,
    out,
    gat,
    send,
    recv,
    win,
    mine,
    reqs,
    offs,
    asked,
    qs,
    acc,
    peak,
    mixed,
    gate,
    kt,
    vt,
    vr,
    sbuf,
    z_send,
    x_send,
    x2_send,
    d_send,
    g_recv,
    a_send,
    a_recv,
    w_send,
    wd_send,
    w_recv,
    fx_send,
    fz_send,
    fd_send,
    f_recv,
    q_send,
    q_recv,
    l_sem,
):
    ctx = lax.axis_index("ctx")
    p = lax.axis_index("pb")
    x = ctx // ZN
    z = lax.rem(ctx, ZN)
    flat = ctx * 2 + p
    other = 1 - p

    def at(dx, dz):
        return lax.rem(x + dx + XN, XN) * ZN + lax.rem(z + dz + ZN, ZN)

    def remote(src, dst, ssem, rsem, c, q):
        return pltpu.make_async_remote_copy(
            src_ref=src,
            dst_ref=dst,
            send_sem=ssem,
            recv_sem=rsem,
            device_id={"ctx": c, "pb": q},
            device_id_type=MESH,
        )

    barrier = pltpu.get_barrier_semaphore()

    def greet(i, carry):
        c = lax.rem(ctx + i // 2, CN)
        q = lax.rem(p + lax.rem(i, 2), 2)
        pl.semaphore_signal(barrier, inc=1, device_id={"ctx": c, "pb": q}, device_id_type=MESH)
        return carry

    lax.fori_loop(1, 2 * CN, greet, 0)

    mine[...] = jnp.full((2, 1, 128), -1, jnp.int32)
    for b in range(2):
        mine[b, :, 0:13] = sel[b]
    reqs[0] = jnp.full((2, 1, 128), -1, jnp.int32)
    for b in range(2):
        reqs[0, b, :, 0:13] = sel[b]
    k0, k1 = pack_keys(sk[...].astype(F32))
    win[0, p, 0:128, :] = k0.astype(BF16)
    win[0, p, 128:192, :] = k1.astype(BF16)
    win[0, p, 192:320, :] = sv[...].astype(F32).T.astype(BF16)
    for k in range(1, 3):

        @pl.when(ctx < k)
        def _():
            win[k] = jnp.zeros((2, PACK, 128), BF16)

    b_at = p * UNIT + lax.broadcasted_iota(jnp.int32, (UNIT, 256), 0)
    j_at = lax.broadcasted_iota(jnp.int32, (UNIT, 256), 1)
    n_row = jnp.broadcast_to(lengths[...], (UNIT, 256)).astype(F32)
    starts = jnp.sum(jnp.where(j_at < b_at, n_row, 0.0), axis=1, keepdims=True)
    counts = jnp.sum(jnp.where(j_at == b_at, n_row, 0.0), axis=1, keepdims=True)
    spread = 1.0 / jnp.sqrt(counts)
    span = ck.shape[0] * SBLK
    step = 512
    total_k = jnp.zeros((UNIT, DK), F32)
    total_v = jnp.zeros((UNIT, DV), F32)
    for t in range(0, span, step):
        pos = (lax.broadcasted_iota(jnp.int32, (UNIT, step), 1) + t).astype(F32)
        away = pos - starts
        member = (away >= 0.0) & (away < counts)
        off = jnp.sum(jnp.where(member, away, 0.0), axis=0, keepdims=True)
        weight = jnp.zeros((1, step), F32)
        for i in range(32):
            weight = jnp.where(off == float(i), cw[0, i], weight)
        matrix = jnp.where(member, weight * spread, 0.0).astype(BF16)
        rows = ck[t // SBLK : (t + step) // SBLK].reshape(step, DK)
        vals = cv[t // SBLK : (t + step) // SBLK].reshape(step, DV)
        total_k += jnp.dot(matrix, rows, preferred_element_type=F32)
        total_v += jnp.dot(matrix, vals, preferred_element_type=F32)
    k0, k1 = pack_keys(total_k)
    gat[0, 0, p, 0:128, :] = k0.astype(BF16)
    gat[0, 0, p, 128:192, :] = k1.astype(BF16)
    gat[0, 0, p, 192:320, :] = total_v.T.astype(BF16)

    pl.semaphore_wait(barrier, 2 * CN - 1)

    def to_q(i):
        dx, dz = i // ZN, lax.rem(i, ZN)
        back = lax.rem(XN - dx, XN) * ZN + lax.rem(ZN - dz, ZN)
        return remote(mine, reqs.at[back], q_send.at[i], q_recv.at[back], at(dx, dz), p)

    def got_q(i, carry):
        remote(mine, reqs.at[i], q_send.at[i], q_recv.at[i], ctx, other).wait_recv()
        return carry

    def start_all(make):
        def one(i, carry):
            make(i).start()
            return carry

        lax.fori_loop(1, CN, one, 0)

    def sent_all(make):
        def one(i, carry):
            make(i).wait_send()
            return carry

        lax.fori_loop(1, CN, one, 0)

    start_all(to_q)

    def g_at(xr, zr, q):
        t, n = slot(xr, zr)
        return gat.at[t, n, q]

    def g_sem(xr, zr, q):
        t, n = slot(xr, zr)
        return g_recv.at[t, n, q]

    def to_z(zr, up):
        return remote(
            g_at(0, zr, p),
            g_at(0, (zr + (7 if up else 1)) % ZN, p),
            z_send.at[zr, 0 if up else 1],
            g_sem(0, (zr + (7 if up else 1)) % ZN, p),
            at(0, 1 if up else -1),
            p,
        )

    def to_x(zr, up):
        return remote(
            g_at(0, zr, p),
            g_at(3 if up else 1, zr, p),
            x_send.at[zr, 0 if up else 1],
            g_sem(3 if up else 1, zr, p),
            at(1 if up else -1, 0),
            p,
        )

    def to_x2(zr):
        t3, n = slot(3, zr)
        t1, _ = slot(1, zr)
        return remote(
            gat.at[t3 + p * (t1 - t3), n, p],
            g_at(2, zr, p),
            x2_send.at[zr],
            g_sem(2, zr, p),
            at(1 - 2 * p, 0),
            p,
        )

    def to_d(xr, zr):
        return remote(
            g_at(xr, zr, p), g_at(xr, zr, p), d_send.at[xr, zr], g_sem(xr, zr, p), ctx, other
        )

    def arrive(xr, zr, q):
        remote(
            g_at(xr, zr, q), g_at(xr, zr, q), d_send.at[xr, zr], g_sem(xr, zr, q), ctx, other
        ).wait_recv()

    def spread_on(zr):
        if zr in (0, 7, 6):
            to_z(zr, True).start()
        if zr in (0, 1, 2):
            to_z(zr, False).start()
        if zr == 5:

            @pl.when(p == 0)
            def _():
                to_z(5, True).start()

        if zr == 3:

            @pl.when(p == 1)
            def _():
                to_z(3, False).start()

        to_x(zr, True).start()
        to_x(zr, False).start()
        to_d(0, zr).start()

    spread_on(0)

    def to_w(k):
        return remote(
            win.at[k, p], win.at[k + 1, p], w_send.at[k], w_recv.at[k + 1, p], lax.rem(ctx + 1, CN), p
        )

    def to_wd(k):
        return remote(win.at[k, p], win.at[k, p], wd_send.at[k], w_recv.at[k, p], ctx, other)

    def got_w(k, q):
        remote(win.at[k, q], win.at[k, q], wd_send.at[k], w_recv.at[k, q], ctx, other).wait_recv()

    @pl.when(ctx + 1 < CN)
    def _():
        to_w(0).start()

    to_wd(0).start()

    def store_block(ref, at_index, number):
        a0, a1 = pack_keys(ck[number].astype(F32))
        ref[at_index, 0:64, :] = a0.astype(BF16)
        ref[at_index, 64:96, :] = a1.astype(BF16)
        ref[at_index, 96:160, :] = cv[number]

    def part(w, q):
        if w:
            return recv.at[65 + q]
        return recv.at[64, pl.ds(pl.multiple_of(q * (SPACK // 2), 16), SPACK // 2)]

    def to_f(w, dx, dz, sem):
        return remote(part(w, p), part(w, p), sem, f_recv.at[w, p], at(dx, dz), p)

    def to_fd(w):
        return remote(part(w, p), part(w, p), fd_send.at[w], f_recv.at[w, p], ctx, other)

    def got_f(w, q):
        remote(part(w, q), part(w, q), fd_send.at[w], f_recv.at[w, q], ctx, other).wait_recv()

    origin, hop, goes_up, goes_down = [], [], [], []
    for ox, oz in ORIGIN:
        away = lax.rem(z - oz + ZN, ZN)
        origin.append((x == ox) & (z == oz))
        hop.append(
            jnp.where(
                away == 0, jnp.where(x == ox, 0, 1), jnp.where(away <= 4, away + 1, 9 - away)
            )
        )
        goes_up.append(away <= 3)
        goes_down.append((away == 0) | (away >= 6))

    def along_z(w, do):
        @pl.when(goes_up[w])
        def _():
            do(to_f(w, 0, 1, fz_send.at[w, 0]))

        @pl.when(goes_down[w])
        def _():
            do(to_f(w, 0, -1, fz_send.at[w, 1]))

    def start(copy):
        copy.start()

    def sent(copy):
        copy.wait_send()

    def from_origin(w):
        for k in range(1, XN):
            to_f(w, k, 0, fx_send.at[w, k - 1]).start()
        along_z(w, start)

    @pl.when(origin[0])
    def _():
        store_block(recv, 64, 0)
        from_origin(0)

    @pl.when(origin[1])
    def _():
        store_block(recv, 65, SBLK - 2)
        store_block(recv, 66, SBLK - 1)
        from_origin(1)

    def fixed(h):
        for w in range(2):

            @pl.when(hop[w] == h)
            def _():
                got_f(w, p)
                to_fd(w).start()
                along_z(w, start)

    lane = lax.broadcasted_iota(jnp.int32, (UNIT, 256), 1)
    for pair in range(HEADS // 2):
        both = queries[:, pair * 384 : (pair + 1) * 384].astype(F32)
        first = jnp.where(lane < DK, both[:, 0:256], 0.0).astype(BF16)
        second = jnp.where(lane < DK, pltpu.roll(both[:, 128:384], 192, 1), 0.0).astype(BF16)
        for h, rows in ((2 * pair, first), (2 * pair + 1, second)):
            for b in range(2):
                base = b * 1024 + h * 64
                qs[base : base + 64, :] = rows[b * 64 : b * 64 + 64]

    lfn = pltpu.make_async_copy(offs, asked, l_sem)
    lax.fori_loop(1, CN, got_q, 0)
    big = 1 << 20
    lanes = lax.broadcasted_iota(jnp.int32, (CN, 1, 128), 2)
    keys = []
    for b in range(2):
        ids = reqs[:, b]
        here = (ids >= ctx * SBLK) & (ids < (ctx + 1) * SBLK)
        keys.append(jnp.where(here, b * 8192 + lanes * SBLK + ids - ctx * SBLK, big))
    one = jnp.min(jnp.minimum(keys[0], keys[1]), axis=2, keepdims=True)
    rest = [jnp.where(k > one, k, big) for k in keys]
    two = jnp.min(jnp.minimum(rest[0], rest[1]), axis=2, keepdims=True)
    offs[...] = jnp.where(lanes == 0, one, two) & (SBLK - 1)
    lfn.start()

    lane = lax.broadcasted_iota(jnp.int32, (8, 128), 1)
    for i in range(3):
        g = jax.nn.sigmoid(gl[i])
        turned = pltpu.roll(g, 64, 1)
        for b in range(2):
            for h in range(0, HEADS, 2):
                low = (g, turned)[b][h : h + 1]
                high = (turned, g)[b][h + 1 : h + 2]
                c, n = b * 2 + h // 8, (h % 8) * 64
                gate[i, c, :, n : n + 128] = jnp.where(lane < 64, low, high)
    vt[128:144, :] = jnp.ones((16, 1024), BF16)

    def unpack_keys(ref_at, n, base):
        half = ref_at[n : n + n // 2, :]
        kt[base : base + n, 0:128] = ref_at[0:n, :]
        kt[base : base + n // 2, 128:256] = half
        kt[base + n // 2 : base + n, 128:256] = pltpu.roll(half.astype(F32), 64, 1).astype(BF16)

    def unpack(ref_at, base):
        unpack_keys(ref_at, UNIT, base)
        vt[0:128, base : base + UNIT] = ref_at[192:320, :]

    lfn.wait()

    def to_a(i):
        dx, dz = i // ZN, lax.rem(i, ZN)
        back = lax.rem(XN - dx, XN) * ZN + lax.rem(ZN - dz, ZN)
        return remote(
            send.at[pl.ds(2 * i, 2)],
            recv.at[pl.ds(2 * back, 2)],
            a_send.at[i],
            a_recv.at[back],
            at(dx, dz),
            p,
        )

    for j in range(2):
        store_block(recv, j, asked[0, 0, j])

    def fill(n, carry):
        i = lax.rem(n * 5, CN)
        for j in range(2):
            store_block(send, 2 * i + j, asked[i, 0, j])
        to_a(i).start()
        return carry

    def listed(stage):
        if not PACE[stage]:
            return
        lax.fori_loop(1 + sum(PACE[:stage]), 1 + sum(PACE[: stage + 1]), fill, 0)

    listed(0)

    for zr in (1, 7):
        arrive(0, zr, p)
        spread_on(zr)

    @pl.when(ctx >= 1)
    def _():
        got_w(1, p)
        to_wd(1).start()

        @pl.when(ctx + 1 < CN)
        def _():
            to_w(1).start()

    listed(1)
    fixed(1)

    for zr in (2, 6):
        arrive(0, zr, p)
        spread_on(zr)
    fixed(2)

    @pl.when(ctx >= 2)
    def _():
        got_w(2, p)
        to_wd(2).start()

    got_w(0, other)
    for k in (1, 2):

        @pl.when(ctx >= k)
        def _():
            got_w(k, other)

    for k in range(5):
        unpack(win.at[2 - (p + k) // 2, lax.rem(p + k, 2)], k * UNIT)
    near = WINDOW + UNIT

    def scores(c, width):
        return dot_t(kt[0:width, :], qs[c * CHUNK : (c + 1) * CHUNK, :])

    def mix(e, width):
        return jnp.dot(vt[:, 0:width], e, preferred_element_type=F32)

    sbuf[0, 0:near, :] = scores(0, near)
    for c in range(4):
        if c < 3:
            sbuf[(c + 1) % 2, 0:near, :] = scores(c + 1, near)
        i_at = lax.broadcasted_iota(jnp.int32, (near, CHUNK), 1) & 63
        j_at = lax.broadcasted_iota(jnp.int32, (near, CHUNK), 0)
        dist = WINDOW + (c // 2) * 64 + i_at - j_at
        allowed = (dist >= 0) & (dist < WINDOW) & (j_at >= WINDOW - flat * UNIT)
        sc = jnp.where(allowed, sbuf[c % 2, 0:near, :] * CEXP, LOW)
        e = jnp.exp2(sc - jnp.max(sc, axis=0, keepdims=True)).astype(BF16)
        o = mix(e, near)
        mixed[c] = o[0:128] * (gate[2, c, 0:1] / o[128:129])
        peak[c] = jnp.full((8, CHUNK), LOW, F32)
        acc[c] = jnp.zeros((144, CHUNK), F32)

    def stage(t):
        if t == 0:
            for zr in (3, 5):
                arrive(0, zr, p)
                spread_on(zr)
            need = [(0, zr) for zr in ZSET[0]]
        elif t == 1:
            arrive(0, 4, p)
            spread_on(4)
            need = [(0, zr) for zr in ZSET[1]]
        else:
            xr, far = ORDER[t]
            need = [(xr, zr) for zr in ZSET[far]]
            if xr == 3:
                for zr in ZSET[far]:
                    arrive(3, zr, p)
                    to_d(3, zr).start()
                    arrive(1, zr, p)
                    to_d(1, zr).start()
                    to_x2(zr).start()
            elif xr == 2:
                for zr in ZSET[far]:
                    arrive(2, zr, p)
                    to_d(2, zr).start()
        if t < 3:
            fixed(t + 3)
        if t < 6:
            listed(t + 2)
        for xr, zr in need:
            arrive(xr, zr, other)

    def tile(t, carry):
        for k in range(8):

            @pl.when(t == k)
            def _():
                stage(k)

        for n in range(4):
            for q in range(2):
                unpack(gat.at[t, n, q], n * 256 + q * UNIT)
        sbuf[0] = scores(0, 1024)
        for c in range(4):
            if c < 3:
                sbuf[(c + 1) % 2] = scores(c + 1, 1024)
            sc = sbuf[c % 2]
            before = peak[c]
            top = jnp.maximum(before, jnp.max(sc, axis=0, keepdims=True) * CEXP)
            e = jnp.exp2(sc * CEXP - top[0:1]).astype(BF16)
            factor = jnp.exp2(before - top)[0:1]
            acc[c] = acc[c] * factor + mix(e, 1024)
            peak[c] = top
        return carry

    lax.fori_loop(0, 8, tile, 0)

    for c in range(4):
        mixed[c] += acc[c, 0:128] * (gate[0, c, 0:1] / acc[c, 128:129])

    def got_a(i, carry):
        remote(
            send.at[pl.ds(2 * i, 2)], recv.at[pl.ds(2 * i, 2)], a_send.at[i], a_recv.at[i], ctx, other
        ).wait_recv()
        return carry

    lax.fori_loop(1, CN, got_a, 0)

    for w in range(2):

        @pl.when(hop[w] > 0)
        def _():
            got_f(w, other)

    ids = [sel_s[b, 0, n] for b in range(2) for n in range(13)]
    owner = [i // SBLK for i in ids]
    picks = []
    for n, own in enumerate(owner):
        rank = 0
        for m in range(n):
            rank = rank + jnp.where(owner[m] == own, 1, 0)
        ox, oz = own // ZN, own % ZN
        rel = ((ox + XN - x) % XN) * ZN + (oz + ZN - z) % ZN
        picks.append(rel * 2 + jnp.minimum(rank, 1))
    for b in range(2):
        for n in range(16):
            number = 64 + n if n < 3 else picks[b * 13 + n - 3]
            block = recv[number]
            unpack_keys(block, SBLK, n * SBLK)
            vr[n * 64 : n * 64 + 64, :] = block[96:160]
        vt[0:128, :] = vr[...].T
        sbuf[0] = scores(2 * b, 1024)
        for r in range(2):
            if r == 0:
                sbuf[1] = scores(2 * b + 1, 1024)
            c = 2 * b + r
            sc = sbuf[r] * CEXP
            e = jnp.exp2(sc - jnp.max(sc, axis=0, keepdims=True)).astype(BF16)
            o = mix(e, 1024)
            done = (mixed[c] + o[0:128] * (gate[1, c, 0:1] / o[128:129])).T
            for h in range(CHUNK // 64):
                head = r * (CHUNK // 64) + h
                out[b * 64 : b * 64 + 64, head * 128 : head * 128 + 128] = done[
                    h * 64 : h * 64 + 64
                ].astype(BF16)

    for zr in (0, 7, 6):
        to_z(zr, True).wait_send()
    for zr in (0, 1, 2):
        to_z(zr, False).wait_send()

    @pl.when(p == 0)
    def _():
        to_z(5, True).wait_send()

    @pl.when(p == 1)
    def _():
        to_z(3, False).wait_send()

    for zr in range(ZN):
        to_x(zr, True).wait_send()
        to_x(zr, False).wait_send()
        to_x2(zr).wait_send()
        for xr in range(XN):
            to_d(xr, zr).wait_send()
    to_wd(0).wait_send()

    @pl.when(ctx + 1 < CN)
    def _():
        to_w(0).wait_send()

    @pl.when(ctx >= 1)
    def _():
        to_wd(1).wait_send()

        @pl.when(ctx + 1 < CN)
        def _():
            to_w(1).wait_send()

    @pl.when(ctx >= 2)
    def _():
        to_wd(2).wait_send()

    sent_all(to_q)
    sent_all(to_a)

    for w in range(2):
        along_z(w, sent)

        @pl.when(hop[w] > 0)
        def _():
            to_fd(w).wait_send()

        @pl.when(origin[w])
        def _():
            for k in range(1, XN):
                to_f(w, k, 0, fx_send.at[w, k - 1]).wait_send()


def on_device(queries, sk, sv, pk, cv, lengths, cw, selections, gl):
    blocks = pk.shape[0] // SBLK
    vmem = pl.BlockSpec(memory_space=pltpu.VMEM)
    smem = pl.BlockSpec(memory_space=pltpu.SMEM)
    dma = pltpu.SemaphoreType.DMA
    return pl.pallas_call(
        body,
        name="attend",
        out_shape=jax.ShapeDtypeStruct((queries.shape[0], HEADS * DV), BF16),
        in_specs=[smem] * 2 + [vmem] * 8,
        out_specs=vmem,
        scratch_shapes=[
            pltpu.VMEM((8, 4, 2, PACK, 128), BF16),
            pltpu.VMEM((2 * CN, SPACK, 128), BF16),
            pltpu.VMEM((2 * CN + 3, SPACK, 128), BF16),
            pltpu.VMEM((3, 2, PACK, 128), BF16),
            pltpu.VMEM((2, 1, 128), jnp.int32),
            pltpu.VMEM((CN, 2, 1, 128), jnp.int32),
            pltpu.VMEM((CN, 1, 128), jnp.int32),
            pltpu.SMEM((CN, 1, 128), jnp.int32),
            pltpu.VMEM((ROWS, 256), BF16),
            pltpu.VMEM((4, 144, CHUNK), F32),
            pltpu.VMEM((4, 8, CHUNK), F32),
            pltpu.VMEM((4, 128, CHUNK), F32),
            pltpu.VMEM((3, 4, 8, CHUNK), F32),
            pltpu.VMEM((1024, 256), BF16),
            pltpu.VMEM((144, 1024), BF16),
            pltpu.VMEM((1024, 128), BF16),
            pltpu.VMEM((2, 1024, CHUNK), F32),
            dma((ZN, 2)),
            dma((ZN, 2)),
            dma((ZN,)),
            dma((XN, ZN)),
            dma((8, 4, 2)),
            dma((CN,)),
            dma((CN,)),
            dma((2,)),
            dma((3,)),
            dma((3, 2)),
            dma((2, 3)),
            dma((2, 2)),
            dma((2,)),
            dma((2, 2)),
            dma((CN,)),
            dma((CN,)),
            dma(()),
        ],
        compiler_params=pltpu.CompilerParams(
            collective_id=0, has_side_effects=True, vmem_limit_bytes=60 * 1024 * 1024
        ),
    )(
        cw,
        selections,
        selections,
        lengths,
        queries,
        sk,
        sv,
        pk.reshape(blocks, SBLK, DK),
        cv.reshape(blocks, SBLK, DV),
        jnp.transpose(gl, (0, 2, 1)),
    )


def solution(mesh):
    placed = (
        P(("ctx", "pb"), "ga"),
        P(("ctx", "pb"), "ga"),
        P(("ctx", "pb"), "ga"),
        P("ctx", "ga"),
        P("ctx", "ga"),
        P("ctx", None),
        P("ga", None),
        P(("ctx", "pb"), "ga", None),
        P(None, ("ctx", "pb"), "ga"),
    )
    return jax.shard_map(
        on_device, mesh=mesh, in_specs=placed, out_specs=P(("ctx", "pb"), "ga"), check_vma=False
    )
```

```python
import functools
import math

import jax
import jax.numpy as jnp
from jax import lax
from jax.experimental import pallas as pl
from jax.experimental.pallas import tpu as pltpu
from jax.sharding import PartitionSpec as P

SBLK = 64
WINDOW = 512
XN, ZN = 4, 8
CN = XN * ZN
HEADS = 16
DK, DV = 192, 128
UNIT = 128
PACK = UNIT * 5 // 2
SPACK = SBLK * 5 // 2
ZSET = ((0, 1, 7, 2), (6, 3, 5, 4))
ORDER = ((0, 0), (0, 1), (3, 0), (1, 0), (3, 1), (1, 1), (2, 0), (2, 1))
PACE = (6, 9, 10, 6, 0, 0, 0, 0)
ORIGIN = ((0, 0), (XN - 1, ZN - 1))
ROWS = 2048
CHUNK = 512
MESH = pl.DeviceIdType.MESH
LOW = -1e30
CEXP = math.log2(math.e) / math.sqrt(DK)
F32 = jnp.float32
BF16 = jnp.bfloat16


def pack_keys(k):
    n = k.shape[0]
    tail = k[:, 128:192]
    return k[:, :128], jnp.concatenate([tail[: n // 2], tail[n // 2 :]], axis=1)


def dot_t(a, b):
    return lax.dot_general(a, b, (((1,), (1,)), ((), ())), preferred_element_type=F32)


def slot(xr, zr):
    far = 0 if zr in ZSET[0] else 1
    return ORDER.index((xr, far)), ZSET[far].index(zr)


def body(
    cw,
    sel_s,
    sel,
    lengths,
    queries,
    sk,
    sv,
    ckt,
    cv,
    gl,
    out,
    ck,
    gat,
    send,
    recv,
    win,
    mine,
    reqs,
    offs,
    asked,
    qs,
    acc,
    peak,
    mixed,
    gate,
    kt,
    vt,
    vr,
    sbuf,
    z_send,
    x_send,
    x2_send,
    d_send,
    g_recv,
    a_send,
    a_recv,
    w_send,
    wd_send,
    w_recv,
    fx_send,
    fz_send,
    fd_send,
    f_recv,
    q_send,
    q_recv,
    l_sem,
):
    ctx = lax.axis_index("ctx")
    p = lax.axis_index("pb")
    x = ctx // ZN
    z = lax.rem(ctx, ZN)
    flat = ctx * 2 + p
    other = 1 - p

    def at(dx, dz):
        return lax.rem(x + dx + XN, XN) * ZN + lax.rem(z + dz + ZN, ZN)

    def remote(src, dst, ssem, rsem, c, q):
        return pltpu.make_async_remote_copy(
            src_ref=src,
            dst_ref=dst,
            send_sem=ssem,
            recv_sem=rsem,
            device_id={"ctx": c, "pb": q},
            device_id_type=MESH,
        )

    barrier = pltpu.get_barrier_semaphore()

    def greet(i, carry):
        c = lax.rem(ctx + i // 2, CN)
        q = lax.rem(p + lax.rem(i, 2), 2)
        pl.semaphore_signal(barrier, inc=1, device_id={"ctx": c, "pb": q}, device_id_type=MESH)
        return carry

    lax.fori_loop(1, 2 * CN, greet, 0)

    mine[...] = jnp.full((2, 1, 128), -1, jnp.int32)
    for b in range(2):
        mine[b, :, 0:13] = sel[b]
    reqs[0] = jnp.full((2, 1, 128), -1, jnp.int32)
    for b in range(2):
        reqs[0, b, :, 0:13] = sel[b]
    k0, k1 = pack_keys(sk[...].astype(F32).T)
    win[0, p, 0:128, :] = k0.astype(BF16)
    win[0, p, 128:192, :] = k1.astype(BF16)
    win[0, p, 192:320, :] = sv[...].astype(F32).T.astype(BF16)
    for k in range(1, 3):

        @pl.when(ctx < k)
        def _():
            win[k] = jnp.zeros((2, PACK, 128), BF16)

    b_at = p * UNIT + lax.broadcasted_iota(jnp.int32, (UNIT, 256), 0)
    j_at = lax.broadcasted_iota(jnp.int32, (UNIT, 256), 1)
    n_row = jnp.broadcast_to(lengths[...], (UNIT, 256)).astype(F32)
    starts = jnp.sum(jnp.where(j_at < b_at, n_row, 0.0), axis=1, keepdims=True)
    counts = jnp.sum(jnp.where(j_at == b_at, n_row, 0.0), axis=1, keepdims=True)
    spread = 1.0 / jnp.sqrt(counts)
    span = ckt.shape[1]
    step = 512
    total_k = jnp.zeros((UNIT, DK), F32)
    total_v = jnp.zeros((UNIT, DV), F32)
    for t in range(0, span, step):
        pos = (lax.broadcasted_iota(jnp.int32, (UNIT, step), 1) + t).astype(F32)
        away = pos - starts
        member = (away >= 0.0) & (away < counts)
        off = jnp.sum(jnp.where(member, away, 0.0), axis=0, keepdims=True)
        weight = jnp.zeros((1, step), F32)
        for i in range(32):
            weight = jnp.where(off == float(i), cw[0, i], weight)
        matrix = jnp.where(member, weight * spread, 0.0).astype(BF16)
        rows = ckt[:, t : t + step].T
        ck[t // SBLK : (t + step) // SBLK] = rows.reshape(step // SBLK, SBLK, DK)
        vals = cv[t // SBLK : (t + step) // SBLK].reshape(step, DV)
        total_k += jnp.dot(matrix, rows, preferred_element_type=F32)
        total_v += jnp.dot(matrix, vals, preferred_element_type=F32)
    k0, k1 = pack_keys(total_k)
    gat[0, 0, p, 0:128, :] = k0.astype(BF16)
    gat[0, 0, p, 128:192, :] = k1.astype(BF16)
    gat[0, 0, p, 192:320, :] = total_v.T.astype(BF16)

    pl.semaphore_wait(barrier, 2 * CN - 1)

    def to_q(i):
        dx, dz = i // ZN, lax.rem(i, ZN)
        back = lax.rem(XN - dx, XN) * ZN + lax.rem(ZN - dz, ZN)
        return remote(mine, reqs.at[back], q_send.at[i], q_recv.at[back], at(dx, dz), p)

    def got_q(i, carry):
        remote(mine, reqs.at[i], q_send.at[i], q_recv.at[i], ctx, other).wait_recv()
        return carry

    def start_all(make):
        def one(i, carry):
            make(i).start()
            return carry

        lax.fori_loop(1, CN, one, 0)

    def sent_all(make):
        def one(i, carry):
            make(i).wait_send()
            return carry

        lax.fori_loop(1, CN, one, 0)

    start_all(to_q)

    def g_at(xr, zr, q):
        t, n = slot(xr, zr)
        return gat.at[t, n, q]

    def g_sem(xr, zr, q):
        t, n = slot(xr, zr)
        return g_recv.at[t, n, q]

    def to_z(zr, up):
        return remote(
            g_at(0, zr, p),
            g_at(0, (zr + (7 if up else 1)) % ZN, p),
            z_send.at[zr, 0 if up else 1],
            g_sem(0, (zr + (7 if up else 1)) % ZN, p),
            at(0, 1 if up else -1),
            p,
        )

    def to_x(zr, up):
        return remote(
            g_at(0, zr, p),
            g_at(3 if up else 1, zr, p),
            x_send.at[zr, 0 if up else 1],
            g_sem(3 if up else 1, zr, p),
            at(1 if up else -1, 0),
            p,
        )

    def to_x2(zr):
        t3, n = slot(3, zr)
        t1, _ = slot(1, zr)
        return remote(
            gat.at[t3 + p * (t1 - t3), n, p],
            g_at(2, zr, p),
            x2_send.at[zr],
            g_sem(2, zr, p),
            at(1 - 2 * p, 0),
            p,
        )

    def to_d(xr, zr):
        return remote(
            g_at(xr, zr, p), g_at(xr, zr, p), d_send.at[xr, zr], g_sem(xr, zr, p), ctx, other
        )

    def arrive(xr, zr, q):
        remote(
            g_at(xr, zr, q), g_at(xr, zr, q), d_send.at[xr, zr], g_sem(xr, zr, q), ctx, other
        ).wait_recv()

    def spread_on(zr):
        if zr in (0, 7, 6):
            to_z(zr, True).start()
        if zr in (0, 1, 2):
            to_z(zr, False).start()
        if zr == 5:

            @pl.when(p == 0)
            def _():
                to_z(5, True).start()

        if zr == 3:

            @pl.when(p == 1)
            def _():
                to_z(3, False).start()

        to_x(zr, True).start()
        to_x(zr, False).start()
        to_d(0, zr).start()

    spread_on(0)

    def to_w(k):
        return remote(
            win.at[k, p], win.at[k + 1, p], w_send.at[k], w_recv.at[k + 1, p], lax.rem(ctx + 1, CN), p
        )

    def to_wd(k):
        return remote(win.at[k, p], win.at[k, p], wd_send.at[k], w_recv.at[k, p], ctx, other)

    def got_w(k, q):
        remote(win.at[k, q], win.at[k, q], wd_send.at[k], w_recv.at[k, q], ctx, other).wait_recv()

    @pl.when(ctx + 1 < CN)
    def _():
        to_w(0).start()

    to_wd(0).start()

    def store_block(ref, at_index, number):
        a0, a1 = pack_keys(ck[number].astype(F32))
        ref[at_index, 0:64, :] = a0.astype(BF16)
        ref[at_index, 64:96, :] = a1.astype(BF16)
        ref[at_index, 96:160, :] = cv[number]

    def part(w, q):
        if w:
            return recv.at[65 + q]
        return recv.at[64, pl.ds(pl.multiple_of(q * (SPACK // 2), 16), SPACK // 2)]

    def to_f(w, dx, dz, sem):
        return remote(part(w, p), part(w, p), sem, f_recv.at[w, p], at(dx, dz), p)

    def to_fd(w):
        return remote(part(w, p), part(w, p), fd_send.at[w], f_recv.at[w, p], ctx, other)

    def got_f(w, q):
        remote(part(w, q), part(w, q), fd_send.at[w], f_recv.at[w, q], ctx, other).wait_recv()

    origin, hop, goes_up, goes_down = [], [], [], []
    for ox, oz in ORIGIN:
        away = lax.rem(z - oz + ZN, ZN)
        origin.append((x == ox) & (z == oz))
        hop.append(
            jnp.where(
                away == 0, jnp.where(x == ox, 0, 1), jnp.where(away <= 4, away + 1, 9 - away)
            )
        )
        goes_up.append(away <= 3)
        goes_down.append((away == 0) | (away >= 6))

    def along_z(w, do):
        @pl.when(goes_up[w])
        def _():
            do(to_f(w, 0, 1, fz_send.at[w, 0]))

        @pl.when(goes_down[w])
        def _():
            do(to_f(w, 0, -1, fz_send.at[w, 1]))

    def start(copy):
        copy.start()

    def sent(copy):
        copy.wait_send()

    def from_origin(w):
        for k in range(1, XN):
            to_f(w, k, 0, fx_send.at[w, k - 1]).start()
        along_z(w, start)

    @pl.when(origin[0])
    def _():
        store_block(recv, 64, 0)
        from_origin(0)

    @pl.when(origin[1])
    def _():
        store_block(recv, 65, SBLK - 2)
        store_block(recv, 66, SBLK - 1)
        from_origin(1)

    def fixed(h):
        for w in range(2):

            @pl.when(hop[w] == h)
            def _():
                got_f(w, p)
                to_fd(w).start()
                along_z(w, start)

    lane = lax.broadcasted_iota(jnp.int32, (UNIT, 256), 1)
    for pair in range(HEADS // 2):
        both = queries[:, pair * 384 : (pair + 1) * 384].astype(F32)
        first = jnp.where(lane < DK, both[:, 0:256], 0.0).astype(BF16)
        second = jnp.where(lane < DK, pltpu.roll(both[:, 128:384], 192, 1), 0.0).astype(BF16)
        for h, rows in ((2 * pair, first), (2 * pair + 1, second)):
            for b in range(2):
                base = b * 1024 + h * 64
                qs[base : base + 64, :] = rows[b * 64 : b * 64 + 64]

    lfn = pltpu.make_async_copy(offs, asked, l_sem)
    lax.fori_loop(1, CN, got_q, 0)
    big = 1 << 20
    lanes = lax.broadcasted_iota(jnp.int32, (CN, 1, 128), 2)
    keys = []
    for b in range(2):
        ids = reqs[:, b]
        here = (ids >= ctx * SBLK) & (ids < (ctx + 1) * SBLK)
        keys.append(jnp.where(here, b * 8192 + lanes * SBLK + ids - ctx * SBLK, big))
    one = jnp.min(jnp.minimum(keys[0], keys[1]), axis=2, keepdims=True)
    rest = [jnp.where(k > one, k, big) for k in keys]
    two = jnp.min(jnp.minimum(rest[0], rest[1]), axis=2, keepdims=True)
    offs[...] = jnp.where(lanes == 0, one, two) & (SBLK - 1)
    lfn.start()

    lane = lax.broadcasted_iota(jnp.int32, (8, 128), 1)
    for i in range(3):
        g = jax.nn.sigmoid(gl[i])
        turned = pltpu.roll(g, 64, 1)
        for b in range(2):
            for h in range(0, HEADS, 2):
                low = (g, turned)[b][h : h + 1]
                high = (turned, g)[b][h + 1 : h + 2]
                c, n = b * 2 + h // 8, (h % 8) * 64
                gate[i, c, :, n : n + 128] = jnp.where(lane < 64, low, high)
    vt[128:144, :] = jnp.ones((16, 1024), BF16)

    def unpack_keys(ref_at, n, base):
        half = ref_at[n : n + n // 2, :]
        kt[base : base + n, 0:128] = ref_at[0:n, :]
        kt[base : base + n // 2, 128:256] = half
        kt[base + n // 2 : base + n, 128:256] = pltpu.roll(half.astype(F32), 64, 1).astype(BF16)

    def unpack(ref_at, base):
        unpack_keys(ref_at, UNIT, base)
        vt[0:128, base : base + UNIT] = ref_at[192:320, :]

    lfn.wait()

    def to_a(i):
        dx, dz = i // ZN, lax.rem(i, ZN)
        back = lax.rem(XN - dx, XN) * ZN + lax.rem(ZN - dz, ZN)
        return remote(
            send.at[pl.ds(2 * i, 2)],
            recv.at[pl.ds(2 * back, 2)],
            a_send.at[i],
            a_recv.at[back],
            at(dx, dz),
            p,
        )

    for j in range(2):
        store_block(recv, j, asked[0, 0, j])

    def fill(n, carry):
        i = lax.rem(n * 5, CN)
        for j in range(2):
            store_block(send, 2 * i + j, asked[i, 0, j])
        to_a(i).start()
        return carry

    def listed(stage):
        if not PACE[stage]:
            return
        lax.fori_loop(1 + sum(PACE[:stage]), 1 + sum(PACE[: stage + 1]), fill, 0)

    listed(0)

    for zr in (1, 7):
        arrive(0, zr, p)
        spread_on(zr)

    @pl.when(ctx >= 1)
    def _():
        got_w(1, p)
        to_wd(1).start()

        @pl.when(ctx + 1 < CN)
        def _():
            to_w(1).start()

    listed(1)
    fixed(1)

    for zr in (2, 6):
        arrive(0, zr, p)
        spread_on(zr)
    fixed(2)

    @pl.when(ctx >= 2)
    def _():
        got_w(2, p)
        to_wd(2).start()

    got_w(0, other)
    for k in (1, 2):

        @pl.when(ctx >= k)
        def _():
            got_w(k, other)

    for k in range(5):
        unpack(win.at[2 - (p + k) // 2, lax.rem(p + k, 2)], k * UNIT)
    near = WINDOW + UNIT

    def scores(c, width):
        return dot_t(kt[0:width, :], qs[c * CHUNK : (c + 1) * CHUNK, :])

    def mix(e, width):
        return jnp.dot(vt[:, 0:width], e, preferred_element_type=F32)

    sbuf[0, 0:near, :] = scores(0, near)
    for c in range(4):
        if c < 3:
            sbuf[(c + 1) % 2, 0:near, :] = scores(c + 1, near)
        i_at = lax.broadcasted_iota(jnp.int32, (near, CHUNK), 1) & 63
        j_at = lax.broadcasted_iota(jnp.int32, (near, CHUNK), 0)
        dist = WINDOW + (c // 2) * 64 + i_at - j_at
        allowed = (dist >= 0) & (dist < WINDOW) & (j_at >= WINDOW - flat * UNIT)
        sc = jnp.where(allowed, sbuf[c % 2, 0:near, :] * CEXP, LOW)
        e = jnp.exp2(sc - jnp.max(sc, axis=0, keepdims=True)).astype(BF16)
        o = mix(e, near)
        mixed[c] = o[0:128] * (gate[2, c, 0:1] / o[128:129])
        peak[c] = jnp.full((8, CHUNK), LOW, F32)
        acc[c] = jnp.zeros((144, CHUNK), F32)

    def stage(t):
        if t == 0:
            for zr in (3, 5):
                arrive(0, zr, p)
                spread_on(zr)
            need = [(0, zr) for zr in ZSET[0]]
        elif t == 1:
            arrive(0, 4, p)
            spread_on(4)
            need = [(0, zr) for zr in ZSET[1]]
        else:
            xr, far = ORDER[t]
            need = [(xr, zr) for zr in ZSET[far]]
            if xr == 3:
                for zr in ZSET[far]:
                    arrive(3, zr, p)
                    to_d(3, zr).start()
                    arrive(1, zr, p)
                    to_d(1, zr).start()
                    to_x2(zr).start()
            elif xr == 2:
                for zr in ZSET[far]:
                    arrive(2, zr, p)
                    to_d(2, zr).start()
        if t < 3:
            fixed(t + 3)
        if t < 6:
            listed(t + 2)
        for xr, zr in need:
            arrive(xr, zr, other)

    def tile(t, carry):
        for k in range(8):

            @pl.when(t == k)
            def _():
                stage(k)

        for n in range(4):
            for q in range(2):
                unpack(gat.at[t, n, q], n * 256 + q * UNIT)
        sbuf[0] = scores(0, 1024)
        for c in range(4):
            if c < 3:
                sbuf[(c + 1) % 2] = scores(c + 1, 1024)
            sc = sbuf[c % 2]
            before = peak[c]
            top = jnp.maximum(before, jnp.max(sc, axis=0, keepdims=True) * CEXP)
            e = jnp.exp2(sc * CEXP - top[0:1]).astype(BF16)
            factor = jnp.exp2(before - top)[0:1]
            acc[c] = acc[c] * factor + mix(e, 1024)
            peak[c] = top
        return carry

    lax.fori_loop(0, 8, tile, 0)

    for c in range(4):
        mixed[c] += acc[c, 0:128] * (gate[0, c, 0:1] / acc[c, 128:129])

    def got_a(i, carry):
        remote(
            send.at[pl.ds(2 * i, 2)], recv.at[pl.ds(2 * i, 2)], a_send.at[i], a_recv.at[i], ctx, other
        ).wait_recv()
        return carry

    lax.fori_loop(1, CN, got_a, 0)

    for w in range(2):

        @pl.when(hop[w] > 0)
        def _():
            got_f(w, other)

    ids = [sel_s[b, 0, n] for b in range(2) for n in range(13)]
    owner = [i // SBLK for i in ids]
    picks = []
    for n, own in enumerate(owner):
        rank = 0
        for m in range(n):
            rank = rank + jnp.where(owner[m] == own, 1, 0)
        ox, oz = own // ZN, own % ZN
        rel = ((ox + XN - x) % XN) * ZN + (oz + ZN - z) % ZN
        picks.append(rel * 2 + jnp.minimum(rank, 1))
    for b in range(2):
        for n in range(16):
            number = 64 + n if n < 3 else picks[b * 13 + n - 3]
            block = recv[number]
            unpack_keys(block, SBLK, n * SBLK)
            vr[n * 64 : n * 64 + 64, :] = block[96:160]
        vt[0:128, :] = vr[...].T
        sbuf[0] = scores(2 * b, 1024)
        for r in range(2):
            if r == 0:
                sbuf[1] = scores(2 * b + 1, 1024)
            c = 2 * b + r
            sc = sbuf[r] * CEXP
            e = jnp.exp2(sc - jnp.max(sc, axis=0, keepdims=True)).astype(BF16)
            o = mix(e, 1024)
            done = (mixed[c] + o[0:128] * (gate[1, c, 0:1] / o[128:129])).T
            for h in range(CHUNK // 64):
                head = r * (CHUNK // 64) + h
                out[b * 64 : b * 64 + 64, head * 128 : head * 128 + 128] = done[
                    h * 64 : h * 64 + 64
                ].astype(BF16)

    for zr in (0, 7, 6):
        to_z(zr, True).wait_send()
    for zr in (0, 1, 2):
        to_z(zr, False).wait_send()

    @pl.when(p == 0)
    def _():
        to_z(5, True).wait_send()

    @pl.when(p == 1)
    def _():
        to_z(3, False).wait_send()

    for zr in range(ZN):
        to_x(zr, True).wait_send()
        to_x(zr, False).wait_send()
        to_x2(zr).wait_send()
        for xr in range(XN):
            to_d(xr, zr).wait_send()
    to_wd(0).wait_send()

    @pl.when(ctx + 1 < CN)
    def _():
        to_w(0).wait_send()

    @pl.when(ctx >= 1)
    def _():
        to_wd(1).wait_send()

        @pl.when(ctx + 1 < CN)
        def _():
            to_w(1).wait_send()

    @pl.when(ctx >= 2)
    def _():
        to_wd(2).wait_send()

    sent_all(to_q)
    sent_all(to_a)

    for w in range(2):
        along_z(w, sent)

        @pl.when(hop[w] > 0)
        def _():
            to_fd(w).wait_send()

        @pl.when(origin[w])
        def _():
            for k in range(1, XN):
                to_f(w, k, 0, fx_send.at[w, k - 1]).wait_send()


def on_device(queries, sk, sv, pk, cv, lengths, cw, selections, gl):
    blocks = pk.shape[0] // SBLK
    vmem = pl.BlockSpec(memory_space=pltpu.VMEM)
    smem = pl.BlockSpec(memory_space=pltpu.SMEM)
    dma = pltpu.SemaphoreType.DMA
    return pl.pallas_call(
        body,
        name="attend",
        out_shape=jax.ShapeDtypeStruct((queries.shape[0], HEADS * DV), BF16),
        in_specs=[smem] * 2 + [vmem] * 8,
        out_specs=vmem,
        scratch_shapes=[
            pltpu.VMEM((blocks, SBLK, DK), BF16),
            pltpu.VMEM((8, 4, 2, PACK, 128), BF16),
            pltpu.VMEM((2 * CN, SPACK, 128), BF16),
            pltpu.VMEM((2 * CN + 3, SPACK, 128), BF16),
            pltpu.VMEM((3, 2, PACK, 128), BF16),
            pltpu.VMEM((2, 1, 128), jnp.int32),
            pltpu.VMEM((CN, 2, 1, 128), jnp.int32),
            pltpu.VMEM((CN, 1, 128), jnp.int32),
            pltpu.SMEM((CN, 1, 128), jnp.int32),
            pltpu.VMEM((ROWS, 256), BF16),
            pltpu.VMEM((4, 144, CHUNK), F32),
            pltpu.VMEM((4, 8, CHUNK), F32),
            pltpu.VMEM((4, 128, CHUNK), F32),
            pltpu.VMEM((3, 4, 8, CHUNK), F32),
            pltpu.VMEM((1024, 256), BF16),
            pltpu.VMEM((144, 1024), BF16),
            pltpu.VMEM((1024, 128), BF16),
            pltpu.VMEM((2, 1024, CHUNK), F32),
            dma((ZN, 2)),
            dma((ZN, 2)),
            dma((ZN,)),
            dma((XN, ZN)),
            dma((8, 4, 2)),
            dma((CN,)),
            dma((CN,)),
            dma((2,)),
            dma((3,)),
            dma((3, 2)),
            dma((2, 3)),
            dma((2, 2)),
            dma((2,)),
            dma((2, 2)),
            dma((CN,)),
            dma((CN,)),
            dma(()),
        ],
        compiler_params=pltpu.CompilerParams(
            collective_id=0, has_side_effects=True, vmem_limit_bytes=60 * 1024 * 1024
        ),
    )(
        cw,
        selections,
        selections,
        lengths,
        queries,
        sk.T,
        sv,
        pk.T,
        cv.reshape(blocks, SBLK, DV),
        jnp.transpose(gl, (0, 2, 1)),
    )


def solution(mesh):
    placed = (
        P(("ctx", "pb"), "ga"),
        P(("ctx", "pb"), "ga"),
        P(("ctx", "pb"), "ga"),
        P("ctx", "ga"),
        P("ctx", "ga"),
        P("ctx", None),
        P("ga", None),
        P(("ctx", "pb"), "ga", None),
        P(None, ("ctx", "pb"), "ga"),
    )
    return jax.shard_map(
        on_device, mesh=mesh, in_specs=placed, out_specs=P(("ctx", "pb"), "ga"), check_vma=False
    )
```

```python
import functools
import math

import jax
import jax.numpy as jnp
from jax import lax
from jax.experimental import pallas as pl
from jax.experimental.pallas import tpu as pltpu
from jax.sharding import PartitionSpec as P

SBLK = 64
WINDOW = 512
XN, ZN = 4, 8
CN = XN * ZN
HEADS = 16
DK, DV = 192, 128
UNIT = 128
PACK = UNIT * 5 // 2
SPACK = SBLK * 5 // 2
ZSET = ((0, 1, 7, 2), (6, 3, 5, 4))
ORDER = ((0, 0), (0, 1), (3, 0), (1, 0), (3, 1), (1, 1), (2, 0), (2, 1))
PACE = (6, 5, 6, 6, 5, 3, 0, 0)
ORIGIN = ((0, 0), (XN - 1, ZN - 1))
ROWS = 2048
CHUNK = 512
MESH = pl.DeviceIdType.MESH
LOW = -1e30
CEXP = math.log2(math.e) / math.sqrt(DK)
F32 = jnp.float32
BF16 = jnp.bfloat16


def pack_keys(k):
    n = k.shape[0]
    tail = k[:, 128:192]
    return k[:, :128], jnp.concatenate([tail[: n // 2], tail[n // 2 :]], axis=1)


def dot_t(a, b):
    return lax.dot_general(a, b, (((1,), (1,)), ((), ())), preferred_element_type=F32)


def slot(xr, zr):
    far = 0 if zr in ZSET[0] else 1
    return ORDER.index((xr, far)), ZSET[far].index(zr)


def body(
    cw,
    sel_s,
    sel,
    lengths,
    queries,
    sk,
    sv,
    ckt,
    cv,
    gl,
    out,
    ck,
    gat,
    send,
    recv,
    win,
    mine,
    reqs,
    offs,
    asked,
    qs,
    acc,
    peak,
    mixed,
    gate,
    kt,
    vt,
    vr,
    sbuf,
    z_send,
    x_send,
    x2_send,
    d_send,
    g_recv,
    a_send,
    a_recv,
    w_send,
    wd_send,
    w_recv,
    fx_send,
    fz_send,
    fd_send,
    f_recv,
    q_send,
    q_recv,
    l_sem,
):
    ctx = lax.axis_index("ctx")
    p = lax.axis_index("pb")
    x = ctx // ZN
    z = lax.rem(ctx, ZN)
    flat = ctx * 2 + p
    other = 1 - p

    def at(dx, dz):
        return lax.rem(x + dx + XN, XN) * ZN + lax.rem(z + dz + ZN, ZN)

    def remote(src, dst, ssem, rsem, c, q):
        return pltpu.make_async_remote_copy(
            src_ref=src,
            dst_ref=dst,
            send_sem=ssem,
            recv_sem=rsem,
            device_id={"ctx": c, "pb": q},
            device_id_type=MESH,
        )

    barrier = pltpu.get_barrier_semaphore()

    def greet(i, carry):
        c = lax.rem(ctx + i // 2, CN)
        q = lax.rem(p + lax.rem(i, 2), 2)
        pl.semaphore_signal(barrier, inc=1, device_id={"ctx": c, "pb": q}, device_id_type=MESH)
        return carry

    lax.fori_loop(1, 2 * CN, greet, 0)

    mine[...] = jnp.full((2, 1, 128), -1, jnp.int32)
    for b in range(2):
        mine[b, :, 0:13] = sel[b]
    reqs[0] = jnp.full((2, 1, 128), -1, jnp.int32)
    for b in range(2):
        reqs[0, b, :, 0:13] = sel[b]
    k0, k1 = pack_keys(sk[...].astype(F32).T)
    win[0, p, 0:128, :] = k0.astype(BF16)
    win[0, p, 128:192, :] = k1.astype(BF16)
    win[0, p, 192:320, :] = sv[...].astype(F32).T.astype(BF16)
    for k in range(1, 3):

        @pl.when(ctx < k)
        def _():
            win[k] = jnp.zeros((2, PACK, 128), BF16)

    pl.semaphore_wait(barrier, 2 * CN - 1)

    def to_q(i):
        dx, dz = i // ZN, lax.rem(i, ZN)
        back = lax.rem(XN - dx, XN) * ZN + lax.rem(ZN - dz, ZN)
        return remote(mine, reqs.at[back], q_send.at[i], q_recv.at[back], at(dx, dz), p)

    def got_q(i, carry):
        remote(mine, reqs.at[i], q_send.at[i], q_recv.at[i], ctx, other).wait_recv()
        return carry

    def start_all(make):
        def one(i, carry):
            make(i).start()
            return carry

        lax.fori_loop(1, CN, one, 0)

    def sent_all(make):
        def one(i, carry):
            make(i).wait_send()
            return carry

        lax.fori_loop(1, CN, one, 0)

    start_all(to_q)

    b_at = p * UNIT + lax.broadcasted_iota(jnp.int32, (UNIT, 256), 0)
    j_at = lax.broadcasted_iota(jnp.int32, (UNIT, 256), 1)
    n_row = jnp.broadcast_to(lengths[...], (UNIT, 256)).astype(F32)
    starts = jnp.sum(jnp.where(j_at < b_at, n_row, 0.0), axis=1, keepdims=True)
    counts = jnp.sum(jnp.where(j_at == b_at, n_row, 0.0), axis=1, keepdims=True)
    spread = 1.0 / jnp.sqrt(counts)
    span = ckt.shape[1]
    step = 512
    total_k = jnp.zeros((UNIT, DK), F32)
    total_v = jnp.zeros((UNIT, DV), F32)
    for t in range(0, span, step):
        pos = (lax.broadcasted_iota(jnp.int32, (UNIT, step), 1) + t).astype(F32)
        away = pos - starts
        member = (away >= 0.0) & (away < counts)
        off = jnp.sum(jnp.where(member, away, 0.0), axis=0, keepdims=True)
        weight = jnp.zeros((1, step), F32)
        for i in range(32):
            weight = jnp.where(off == float(i), cw[0, i], weight)
        matrix = jnp.where(member, weight * spread, 0.0).astype(BF16)
        rows = ckt[:, t : t + step].T
        ck[t // SBLK : (t + step) // SBLK] = rows.reshape(step // SBLK, SBLK, DK)
        vals = cv[t // SBLK : (t + step) // SBLK].reshape(step, DV)
        total_k += jnp.dot(matrix, rows, preferred_element_type=F32)
        total_v += jnp.dot(matrix, vals, preferred_element_type=F32)
    k0, k1 = pack_keys(total_k)
    gat[0, 0, p, 0:128, :] = k0.astype(BF16)
    gat[0, 0, p, 128:192, :] = k1.astype(BF16)
    gat[0, 0, p, 192:320, :] = total_v.T.astype(BF16)

    def g_at(xr, zr, q):
        t, n = slot(xr, zr)
        return gat.at[t, n, q]

    def g_sem(xr, zr, q):
        t, n = slot(xr, zr)
        return g_recv.at[t, n, q]

    def to_z(zr, up):
        return remote(
            g_at(0, zr, p),
            g_at(0, (zr + (7 if up else 1)) % ZN, p),
            z_send.at[zr, 0 if up else 1],
            g_sem(0, (zr + (7 if up else 1)) % ZN, p),
            at(0, 1 if up else -1),
            p,
        )

    def to_x(zr, up):
        return remote(
            g_at(0, zr, p),
            g_at(3 if up else 1, zr, p),
            x_send.at[zr, 0 if up else 1],
            g_sem(3 if up else 1, zr, p),
            at(1 if up else -1, 0),
            p,
        )

    def to_x2(zr):
        t3, n = slot(3, zr)
        t1, _ = slot(1, zr)
        return remote(
            gat.at[t3 + p * (t1 - t3), n, p],
            g_at(2, zr, p),
            x2_send.at[zr],
            g_sem(2, zr, p),
            at(1 - 2 * p, 0),
            p,
        )

    def to_d(xr, zr):
        return remote(
            g_at(xr, zr, p), g_at(xr, zr, p), d_send.at[xr, zr], g_sem(xr, zr, p), ctx, other
        )

    def arrive(xr, zr, q):
        remote(
            g_at(xr, zr, q), g_at(xr, zr, q), d_send.at[xr, zr], g_sem(xr, zr, q), ctx, other
        ).wait_recv()

    def spread_on(zr):
        if zr in (0, 7, 6):
            to_z(zr, True).start()
        if zr in (0, 1, 2):
            to_z(zr, False).start()
        if zr == 5:

            @pl.when(p == 0)
            def _():
                to_z(5, True).start()

        if zr == 3:

            @pl.when(p == 1)
            def _():
                to_z(3, False).start()

        to_x(zr, True).start()
        to_x(zr, False).start()
        to_d(0, zr).start()

    spread_on(0)

    def to_w(k):
        return remote(
            win.at[k, p], win.at[k + 1, p], w_send.at[k], w_recv.at[k + 1, p], lax.rem(ctx + 1, CN), p
        )

    def to_wd(k):
        return remote(win.at[k, p], win.at[k, p], wd_send.at[k], w_recv.at[k, p], ctx, other)

    def got_w(k, q):
        remote(win.at[k, q], win.at[k, q], wd_send.at[k], w_recv.at[k, q], ctx, other).wait_recv()

    @pl.when(ctx + 1 < CN)
    def _():
        to_w(0).start()

    to_wd(0).start()

    def store_block(ref, at_index, number):
        a0, a1 = pack_keys(ck[number].astype(F32))
        ref[at_index, 0:64, :] = a0.astype(BF16)
        ref[at_index, 64:96, :] = a1.astype(BF16)
        ref[at_index, 96:160, :] = cv[number]

    def part(w, q):
        if w:
            return recv.at[65 + q]
        return recv.at[64, pl.ds(pl.multiple_of(q * (SPACK // 2), 16), SPACK // 2)]

    def to_f(w, dx, dz, sem):
        return remote(part(w, p), part(w, p), sem, f_recv.at[w, p], at(dx, dz), p)

    def to_fd(w):
        return remote(part(w, p), part(w, p), fd_send.at[w], f_recv.at[w, p], ctx, other)

    def got_f(w, q):
        remote(part(w, q), part(w, q), fd_send.at[w], f_recv.at[w, q], ctx, other).wait_recv()

    origin, hop, goes_up, goes_down = [], [], [], []
    for ox, oz in ORIGIN:
        away = lax.rem(z - oz + ZN, ZN)
        origin.append((x == ox) & (z == oz))
        hop.append(
            jnp.where(
                away == 0, jnp.where(x == ox, 0, 1), jnp.where(away <= 4, away + 1, 9 - away)
            )
        )
        goes_up.append(away <= 3)
        goes_down.append((away == 0) | (away >= 6))

    def along_z(w, do):
        @pl.when(goes_up[w])
        def _():
            do(to_f(w, 0, 1, fz_send.at[w, 0]))

        @pl.when(goes_down[w])
        def _():
            do(to_f(w, 0, -1, fz_send.at[w, 1]))

    def start(copy):
        copy.start()

    def sent(copy):
        copy.wait_send()

    def from_origin(w):
        for k in range(1, XN):
            to_f(w, k, 0, fx_send.at[w, k - 1]).start()
        along_z(w, start)

    @pl.when(origin[0])
    def _():
        store_block(recv, 64, 0)
        from_origin(0)

    @pl.when(origin[1])
    def _():
        store_block(recv, 65, SBLK - 2)
        store_block(recv, 66, SBLK - 1)
        from_origin(1)

    def fixed(h):
        for w in range(2):

            @pl.when(hop[w] == h)
            def _():
                got_f(w, p)
                to_fd(w).start()
                along_z(w, start)

    lfn = pltpu.make_async_copy(offs, asked, l_sem)
    lax.fori_loop(1, CN, got_q, 0)
    big = 1 << 20
    lanes = lax.broadcasted_iota(jnp.int32, (CN, 1, 128), 2)
    keys = []
    for b in range(2):
        ids = reqs[:, b]
        here = (ids >= ctx * SBLK) & (ids < (ctx + 1) * SBLK)
        keys.append(jnp.where(here, b * 8192 + lanes * SBLK + ids - ctx * SBLK, big))
    one = jnp.min(jnp.minimum(keys[0], keys[1]), axis=2, keepdims=True)
    rest = [jnp.where(k > one, k, big) for k in keys]
    two = jnp.min(jnp.minimum(rest[0], rest[1]), axis=2, keepdims=True)
    offs[...] = jnp.where(lanes == 0, one, two) & (SBLK - 1)
    lfn.start()

    lane = lax.broadcasted_iota(jnp.int32, (8, 128), 1)
    for i in range(3):
        g = jax.nn.sigmoid(gl[i])
        turned = pltpu.roll(g, 64, 1)
        for b in range(2):
            for h in range(0, HEADS, 2):
                low = (g, turned)[b][h : h + 1]
                high = (turned, g)[b][h + 1 : h + 2]
                c, n = b * 2 + h // 8, (h % 8) * 64
                gate[i, c, :, n : n + 128] = jnp.where(lane < 64, low, high)
    vt[128:144, :] = jnp.ones((16, 1024), BF16)

    def unpack_keys(ref_at, n, base):
        half = ref_at[n : n + n // 2, :]
        kt[base : base + n, 0:128] = ref_at[0:n, :]
        kt[base : base + n // 2, 128:256] = half
        kt[base + n // 2 : base + n, 128:256] = pltpu.roll(half.astype(F32), 64, 1).astype(BF16)

    def unpack(ref_at, base):
        unpack_keys(ref_at, UNIT, base)
        vt[0:128, base : base + UNIT] = ref_at[192:320, :]

    lfn.wait()

    def to_a(i):
        dx, dz = i // ZN, lax.rem(i, ZN)
        back = lax.rem(XN - dx, XN) * ZN + lax.rem(ZN - dz, ZN)
        return remote(
            send.at[pl.ds(2 * i, 2)],
            recv.at[pl.ds(2 * back, 2)],
            a_send.at[i],
            a_recv.at[back],
            at(dx, dz),
            p,
        )

    for j in range(2):
        store_block(recv, j, asked[0, 0, j])

    def fill(n, carry):
        i = lax.rem(n * 5, CN)
        for j in range(2):
            store_block(send, 2 * i + j, asked[i, 0, j])
        to_a(i).start()
        return carry

    def listed(stage):
        if not PACE[stage]:
            return
        lax.fori_loop(1 + sum(PACE[:stage]), 1 + sum(PACE[: stage + 1]), fill, 0)

    listed(0)

    lane = lax.broadcasted_iota(jnp.int32, (UNIT, 256), 1)
    for pair in range(HEADS // 2):
        both = queries[:, pair * 384 : (pair + 1) * 384].astype(F32)
        first = jnp.where(lane < DK, both[:, 0:256], 0.0).astype(BF16)
        second = jnp.where(lane < DK, pltpu.roll(both[:, 128:384], 192, 1), 0.0).astype(BF16)
        for h, rows in ((2 * pair, first), (2 * pair + 1, second)):
            for b in range(2):
                base = b * 1024 + h * 64
                qs[base : base + 64, :] = rows[b * 64 : b * 64 + 64]


    for zr in (1, 7):
        arrive(0, zr, p)
        spread_on(zr)

    @pl.when(ctx >= 1)
    def _():
        got_w(1, p)
        to_wd(1).start()

        @pl.when(ctx + 1 < CN)
        def _():
            to_w(1).start()

    listed(1)
    fixed(1)

    for zr in (2, 6):
        arrive(0, zr, p)
        spread_on(zr)
    fixed(2)

    @pl.when(ctx >= 2)
    def _():
        got_w(2, p)
        to_wd(2).start()

    got_w(0, other)
    for k in (1, 2):

        @pl.when(ctx >= k)
        def _():
            got_w(k, other)

    for k in range(5):
        unpack(win.at[2 - (p + k) // 2, lax.rem(p + k, 2)], k * UNIT)
    near = WINDOW + UNIT

    def scores(c, width):
        return dot_t(kt[0:width, :], qs[c * CHUNK : (c + 1) * CHUNK, :])

    def mix(e, width):
        return jnp.dot(vt[:, 0:width], e, preferred_element_type=F32)

    sbuf[0, 0:near, :] = scores(0, near)
    for c in range(4):
        if c < 3:
            sbuf[(c + 1) % 2, 0:near, :] = scores(c + 1, near)
        i_at = lax.broadcasted_iota(jnp.int32, (near, CHUNK), 1) & 63
        j_at = lax.broadcasted_iota(jnp.int32, (near, CHUNK), 0)
        dist = WINDOW + (c // 2) * 64 + i_at - j_at
        allowed = (dist >= 0) & (dist < WINDOW) & (j_at >= WINDOW - flat * UNIT)
        sc = jnp.where(allowed, sbuf[c % 2, 0:near, :] * CEXP, LOW)
        e = jnp.exp2(sc - jnp.max(sc, axis=0, keepdims=True)).astype(BF16)
        o = mix(e, near)
        mixed[c] = o[0:128] * (gate[2, c, 0:1] / o[128:129])
        peak[c] = jnp.full((8, CHUNK), LOW, F32)
        acc[c] = jnp.zeros((144, CHUNK), F32)

    def stage(t):
        if t == 0:
            for zr in (3, 5):
                arrive(0, zr, p)
                spread_on(zr)
            need = [(0, zr) for zr in ZSET[0]]
        elif t == 1:
            arrive(0, 4, p)
            spread_on(4)
            need = [(0, zr) for zr in ZSET[1]]
        else:
            xr, far = ORDER[t]
            need = [(xr, zr) for zr in ZSET[far]]
            if xr == 3:
                for zr in ZSET[far]:
                    arrive(3, zr, p)
                    to_d(3, zr).start()
                    arrive(1, zr, p)
                    to_d(1, zr).start()
                    to_x2(zr).start()
            elif xr == 2:
                for zr in ZSET[far]:
                    arrive(2, zr, p)
                    to_d(2, zr).start()
        if t < 3:
            fixed(t + 3)
        if t < 6:
            listed(t + 2)
        for xr, zr in need:
            arrive(xr, zr, other)

    def tile(t, carry):
        for k in range(8):

            @pl.when(t == k)
            def _():
                stage(k)

        for n in range(4):
            for q in range(2):
                unpack(gat.at[t, n, q], n * 256 + q * UNIT)
        sbuf[0] = scores(0, 1024)
        for c in range(4):
            if c < 3:
                sbuf[(c + 1) % 2] = scores(c + 1, 1024)
            sc = sbuf[c % 2]
            before = peak[c]
            top = jnp.maximum(before, jnp.max(sc, axis=0, keepdims=True) * CEXP)
            e = jnp.exp2(sc * CEXP - top[0:1]).astype(BF16)
            factor = jnp.exp2(before - top)[0:1]
            acc[c] = acc[c] * factor + mix(e, 1024)
            peak[c] = top
        return carry

    lax.fori_loop(0, 8, tile, 0)

    for c in range(4):
        mixed[c] += acc[c, 0:128] * (gate[0, c, 0:1] / acc[c, 128:129])

    def got_a(i, carry):
        remote(
            send.at[pl.ds(2 * i, 2)], recv.at[pl.ds(2 * i, 2)], a_send.at[i], a_recv.at[i], ctx, other
        ).wait_recv()
        return carry

    lax.fori_loop(1, CN, got_a, 0)

    for w in range(2):

        @pl.when(hop[w] > 0)
        def _():
            got_f(w, other)

    ids = [sel_s[b, 0, n] for b in range(2) for n in range(13)]
    owner = [i // SBLK for i in ids]
    picks = []
    for n, own in enumerate(owner):
        rank = 0
        for m in range(n):
            rank = rank + jnp.where(owner[m] == own, 1, 0)
        ox, oz = own // ZN, own % ZN
        rel = ((ox + XN - x) % XN) * ZN + (oz + ZN - z) % ZN
        picks.append(rel * 2 + jnp.minimum(rank, 1))
    for b in range(2):
        for n in range(16):
            number = 64 + n if n < 3 else picks[b * 13 + n - 3]
            block = recv[number]
            unpack_keys(block, SBLK, n * SBLK)
            vr[n * 64 : n * 64 + 64, :] = block[96:160]
        vt[0:128, :] = vr[...].T
        sbuf[0] = scores(2 * b, 1024)
        for r in range(2):
            if r == 0:
                sbuf[1] = scores(2 * b + 1, 1024)
            c = 2 * b + r
            sc = sbuf[r] * CEXP
            e = jnp.exp2(sc - jnp.max(sc, axis=0, keepdims=True)).astype(BF16)
            o = mix(e, 1024)
            done = (mixed[c] + o[0:128] * (gate[1, c, 0:1] / o[128:129])).T
            for h in range(CHUNK // 64):
                head = r * (CHUNK // 64) + h
                out[b * 64 : b * 64 + 64, head * 128 : head * 128 + 128] = done[
                    h * 64 : h * 64 + 64
                ].astype(BF16)

    for zr in (0, 7, 6):
        to_z(zr, True).wait_send()
    for zr in (0, 1, 2):
        to_z(zr, False).wait_send()

    @pl.when(p == 0)
    def _():
        to_z(5, True).wait_send()

    @pl.when(p == 1)
    def _():
        to_z(3, False).wait_send()

    for zr in range(ZN):
        to_x(zr, True).wait_send()
        to_x(zr, False).wait_send()
        to_x2(zr).wait_send()
        for xr in range(XN):
            to_d(xr, zr).wait_send()
    to_wd(0).wait_send()

    @pl.when(ctx + 1 < CN)
    def _():
        to_w(0).wait_send()

    @pl.when(ctx >= 1)
    def _():
        to_wd(1).wait_send()

        @pl.when(ctx + 1 < CN)
        def _():
            to_w(1).wait_send()

    @pl.when(ctx >= 2)
    def _():
        to_wd(2).wait_send()

    sent_all(to_q)
    sent_all(to_a)

    for w in range(2):
        along_z(w, sent)

        @pl.when(hop[w] > 0)
        def _():
            to_fd(w).wait_send()

        @pl.when(origin[w])
        def _():
            for k in range(1, XN):
                to_f(w, k, 0, fx_send.at[w, k - 1]).wait_send()


def on_device(queries, sk, sv, pk, cv, lengths, cw, selections, gl):
    blocks = pk.shape[0] // SBLK
    vmem = pl.BlockSpec(memory_space=pltpu.VMEM)
    smem = pl.BlockSpec(memory_space=pltpu.SMEM)
    dma = pltpu.SemaphoreType.DMA
    return pl.pallas_call(
        body,
        name="attend",
        out_shape=jax.ShapeDtypeStruct((queries.shape[0], HEADS * DV), BF16),
        in_specs=[smem] * 2 + [vmem] * 8,
        out_specs=vmem,
        scratch_shapes=[
            pltpu.VMEM((blocks, SBLK, DK), BF16),
            pltpu.VMEM((8, 4, 2, PACK, 128), BF16),
            pltpu.VMEM((2 * CN, SPACK, 128), BF16),
            pltpu.VMEM((2 * CN + 3, SPACK, 128), BF16),
            pltpu.VMEM((3, 2, PACK, 128), BF16),
            pltpu.VMEM((2, 1, 128), jnp.int32),
            pltpu.VMEM((CN, 2, 1, 128), jnp.int32),
            pltpu.VMEM((CN, 1, 128), jnp.int32),
            pltpu.SMEM((CN, 1, 128), jnp.int32),
            pltpu.VMEM((ROWS, 256), BF16),
            pltpu.VMEM((4, 144, CHUNK), F32),
            pltpu.VMEM((4, 8, CHUNK), F32),
            pltpu.VMEM((4, 128, CHUNK), F32),
            pltpu.VMEM((3, 4, 8, CHUNK), F32),
            pltpu.VMEM((1024, 256), BF16),
            pltpu.VMEM((144, 1024), BF16),
            pltpu.VMEM((1024, 128), BF16),
            pltpu.VMEM((2, 1024, CHUNK), F32),
            dma((ZN, 2)),
            dma((ZN, 2)),
            dma((ZN,)),
            dma((XN, ZN)),
            dma((8, 4, 2)),
            dma((CN,)),
            dma((CN,)),
            dma((2,)),
            dma((3,)),
            dma((3, 2)),
            dma((2, 3)),
            dma((2, 2)),
            dma((2,)),
            dma((2, 2)),
            dma((CN,)),
            dma((CN,)),
            dma(()),
        ],
        compiler_params=pltpu.CompilerParams(
            collective_id=0, has_side_effects=True, vmem_limit_bytes=60 * 1024 * 1024
        ),
    )(
        cw,
        selections,
        selections,
        lengths,
        queries,
        sk.T,
        sv,
        pk.T,
        cv.reshape(blocks, SBLK, DV),
        jnp.transpose(gl, (0, 2, 1)),
    )


def solution(mesh):
    placed = (
        P(("ctx", "pb"), "ga"),
        P(("ctx", "pb"), "ga"),
        P(("ctx", "pb"), "ga"),
        P("ctx", "ga"),
        P("ctx", "ga"),
        P("ctx", None),
        P("ga", None),
        P(("ctx", "pb"), "ga", None),
        P(None, ("ctx", "pb"), "ga"),
    )
    return jax.shard_map(
        on_device, mesh=mesh, in_specs=placed, out_specs=P(("ctx", "pb"), "ga"), check_vma=False
    )
```
